16 devices in a mesh: dp: 2 (over z), col: 2 (over y), row: 4 (over x, core).
Axes of the slice: x: 2, y: 2, z: 2, core: 2. Of those that a mesh axis runs over, the one named last changes fastest.
Arguments:
- x_attn: bfloat16 [16384, 1024], P('dp', 'row')
- dy_attn: bfloat16 [16384, 1024], P('dp', 'col')
- x_mlp: bfloat16 [16384, 1024], P('dp', 'row')
- dy_gate: bfloat16 [16384, 4096], P('dp', 'col')
- dy_up: bfloat16 [16384, 4096], P('dp', 'col')
- h_mlp: bfloat16 [16384, 4096], P('dp', 'row')
- dy_out: bfloat16 [16384, 1024], P('dp', 'col')
- w_attn: float32 [1024, 1024], P('row', 'col')
- w_gate: float32 [1024, 4096], P('row', 'col')
- w_up: float32 [1024, 4096], P('row', 'col')
- w_down: float32 [4096, 1024], P('row', 'col')
- r_attn: float32 [1024], P('row')
- c_attn: float32 [1024], P('col')
- r_gate: float32 [1024], P('row')
- c_gate: float32 [4096], P('col')
- r_up: float32 [1024], P('row')
- c_up: float32 [4096], P('col')
- r_down: float32 [4096], P('row')
- c_down: float32 [1024], P('col')
- hyper_params: float32 [3], replicated
Outputs:
- output 1: float32 [1024, 1024], P('row', 'col')
- output 2: float32 [1024], P('row')
- output 3: float32 [1024], P('col')
- output 4: float32 [1024, 4096], P('row', 'col')
- output 5: float32 [1024], P('row')
- output 6: float32 [4096], P('col')
- output 7: float32 [1024, 4096], P('row', 'col')
- output 8: float32 [1024], P('row')
- output 9: float32 [4096], P('col')
- output 10: float32 [4096, 1024], P('row', 'col')
- output 11: float32 [4096], P('row')
- output 12: float32 [1024], P('col')
All inputs are finite; a program needn't handle non-finite values.
Results may differ from the reference program's by a relative error of at most 0.001.
Values are sent between devices in bfloat16 or wider.
A program may use at most 1 GiB of HBM per device.

```python
import jax
import jax.numpy as jnp

D_MODEL = 1024
D_FF = 4096
TOKENS = 16384

EPS_ONE = 1e-30
EPS_TWO = 1e-3


def draw_act(key, rows, cols, scale):
    k_val, k_slope, k_one, k_two = jax.random.split(key, 4)
    position = jnp.linspace(-1.0, 1.0, cols)
    slope_val = jax.random.uniform(k_slope, (), jnp.float32, 0.8, 1.2)
    up_scale = jnp.exp(0.5 * slope_val * position) * jax.random.uniform(k_one, (cols,), jnp.float32, 0.7, 1.3)
    down_scale = jnp.exp(-0.5 * slope_val * position) * jax.random.uniform(k_two, (cols,), jnp.float32, 0.7, 1.3)
    group_scale = jnp.stack([up_scale, down_scale])
    values = jax.random.normal(k_val, (2, rows // 2, cols), jnp.float32) * group_scale[:, None, :]
    return (values.reshape(rows, cols) * scale).astype(jnp.bfloat16)


def draw_weight(key, rows, cols):
    k_val, k_row, k_col = jax.random.split(key, 3)
    row_trend = jax.random.uniform(k_row, (), jnp.float32, 0.8, 1.2) * jnp.linspace(-0.5, 0.5, rows)
    col_trend = jax.random.uniform(k_col, (), jnp.float32, 0.8, 1.2) * jnp.linspace(-0.5, 0.5, cols)
    values = jax.random.normal(k_val, (rows, cols), jnp.float32) * jnp.exp(row_trend[:, None] + col_trend[None, :])
    return values * rows ** -0.5


def draw_stat(key, length):
    return jax.random.uniform(key, (length,), jnp.float32, 0.2, 0.8)


def setup_inputs(seed: int = 0) -> dict:
    key_list = jax.random.split(jax.random.key(seed), 20)
    dy_scale = TOKENS ** -0.5
    hyper_keys = jax.random.split(key_list[19], 3)
    hyper_params = jnp.stack([
        jax.random.uniform(hyper_keys[0], (), jnp.float32, 0.5, 0.9),
        jax.random.uniform(hyper_keys[1], (), jnp.float32, 0.5, 1.0),
        jax.random.uniform(hyper_keys[2], (), jnp.float32, 0.3, 0.6)])
    return {
        'x_attn': draw_act(key_list[0], TOKENS, D_MODEL, 1.0),
        'dy_attn': draw_act(key_list[1], TOKENS, D_MODEL, dy_scale),
        'x_mlp': draw_act(key_list[2], TOKENS, D_MODEL, 1.0),
        'dy_gate': draw_act(key_list[3], TOKENS, D_FF, dy_scale),
        'dy_up': draw_act(key_list[4], TOKENS, D_FF, dy_scale),
        'h_mlp': draw_act(key_list[5], TOKENS, D_FF, 1.0),
        'dy_out': draw_act(key_list[6], TOKENS, D_MODEL, dy_scale),
        'w_attn': draw_weight(key_list[7], D_MODEL, D_MODEL),
        'w_gate': draw_weight(key_list[8], D_MODEL, D_FF),
        'w_up': draw_weight(key_list[9], D_MODEL, D_FF),
        'w_down': draw_weight(key_list[10], D_FF, D_MODEL),
        'r_attn': draw_stat(key_list[11], D_MODEL),
        'c_attn': draw_stat(key_list[12], D_MODEL),
        'r_gate': draw_stat(key_list[13], D_MODEL),
        'c_gate': draw_stat(key_list[14], D_FF),
        'r_up': draw_stat(key_list[15], D_MODEL),
        'c_up': draw_stat(key_list[16], D_FF),
        'r_down': draw_stat(key_list[17], D_FF),
        'c_down': draw_stat(key_list[18], D_MODEL),
        'hyper_params': hyper_params,
    }


def adafactor_step(x_act, dy_act, weight, row_old, col_old, hyper_params):
    beta_two = hyper_params[0]
    rho_step = hyper_params[1]
    clip_thr = hyper_params[2]
    full_grad = jnp.dot(x_act.T, dy_act, preferred_element_type=jnp.float32)
    sq_grad = full_grad * full_grad + EPS_ONE
    new_row = beta_two * row_old + (1.0 - beta_two) * jnp.mean(sq_grad, axis=1)
    new_col = beta_two * col_old + (1.0 - beta_two) * jnp.mean(sq_grad, axis=0)
    row_total = jnp.sum(new_row)
    second_est = new_row[:, None] * new_col[None, :] / row_total
    update = full_grad / jnp.sqrt(second_est)
    upd_rms = jnp.sqrt(jnp.mean(update * update))
    update = update / jnp.maximum(1.0, upd_rms / clip_thr)
    w_rms = jnp.sqrt(jnp.mean(weight * weight))
    step_size = rho_step * jnp.maximum(EPS_TWO, w_rms)
    return (weight - step_size * update, new_row, new_col)


def reference(x_attn, dy_attn, x_mlp, dy_gate, dy_up, h_mlp, dy_out, w_attn, w_gate, w_up, w_down,
              r_attn, c_attn, r_gate, c_gate, r_up, c_up, r_down, c_down, hyper_params):
    attn_res = adafactor_step(x_attn, dy_attn, w_attn, r_attn, c_attn, hyper_params)
    gate_res = adafactor_step(x_mlp, dy_gate, w_gate, r_gate, c_gate, hyper_params)
    up_res = adafactor_step(x_mlp, dy_up, w_up, r_up, c_up, hyper_params)
    down_res = adafactor_step(h_mlp, dy_out, w_down, r_down, c_down, hyper_params)
    return (attn_res[0], attn_res[1], attn_res[2], gate_res[0], gate_res[1], gate_res[2],
            up_res[0], up_res[1], up_res[2], down_res[0], down_res[1], down_res[2])
```

```python
import functools
import math

import jax
import jax.numpy as jnp
from jax import lax
from jax.experimental import pallas as pl
from jax.experimental.pallas import tpu as pltpu
from jax.sharding import PartitionSpec as P

EPS_ONE = 1e-30
EPS_TWO = 1e-3
MESH = pl.DeviceIdType.MESH
F32 = jnp.float32

TM, TN = 256, 512
KC = 1024
NB = 8
RB = 32
LANES = 128


def fold_lanes(v):
    total = v[:, :LANES]
    for j in range(LANES, v.shape[1], LANES):
        total = total + v[:, j:j + LANES]
    return total


def fold_rows(v):
    total = v[:8]
    for i in range(8, v.shape[0], 8):
        total = total + v[i:i + 8]
    return total


def kernel(geo, x_refs, dy_refs, w_refs, r_refs, c_refs, hyper, w_outs, r_outs, c_outs,
           xbuf, ybuf, part, peer, rowpart, acol, brow, msg_one, msg_two,
           x_sem, y_sem, w_sem, bulk_send, bulk_recv, one_send, one_recv, two_send, two_recv):
    n_col, n_row, n_chunk = geo.n_col, geo.n_row, geo.n_chunk
    plane = n_col * n_row
    dp, col, row = lax.axis_index("dp"), lax.axis_index("col"), lax.axis_index("row")
    me = col * n_row + row

    def plane_peer(step):
        other = lax.rem(me + step, plane)
        return other, (dp, lax.div(other, n_row), lax.rem(other, n_row))

    across = (1 - dp, col, row)

    def load(tile, k, slot):
        rows = pl.ds(pl.multiple_of(k * KC, KC), KC)
        for first, count, m_tiles, x_ref, y_ref in geo.groups(x_refs, dy_refs):
            @pl.when(jnp.logical_and(tile >= first, tile < first + count))
            def _():
                local = tile - first
                m_at = local if m_tiles > 1 else 0
                n_at = 0 if m_tiles > 1 else local
                pltpu.make_async_copy(
                    x_ref.at[rows, pl.ds(pl.multiple_of(m_at * TM, TM), TM)], xbuf.at[slot], x_sem.at[slot]).start()
                pltpu.make_async_copy(
                    y_ref.at[rows, pl.ds(pl.multiple_of(n_at * TN, TN), TN)], ybuf.at[slot], y_sem.at[slot]).start()

    def load_done(slot):
        pltpu.make_async_copy(x_refs[0].at[pl.ds(0, KC), pl.ds(0, TM)], xbuf.at[slot], x_sem.at[slot]).wait()
        pltpu.make_async_copy(dy_refs[0].at[pl.ds(0, KC), pl.ds(0, TN)], ybuf.at[slot], y_sem.at[slot]).wait()

    total_chunks = geo.n_tiles * n_chunk
    for c in range(NB - 1):
        load(c // n_chunk, c % n_chunk, c)

    barrier = pltpu.get_barrier_semaphore()
    for step in range(1, plane):
        pl.semaphore_signal(barrier, inc=1, device_id=plane_peer(step)[1], device_id_type=MESH)
    pl.semaphore_signal(barrier, inc=1, device_id=across, device_id_type=MESH)
    w_copies = [pltpu.make_async_copy(w_refs[i], w_outs[i], w_sem.at[i]) for i in range(4)]

    def bulk(tile):
        return pltpu.make_async_remote_copy(
            src_ref=part.at[tile], dst_ref=peer.at[tile], send_sem=bulk_send.at[tile], recv_sem=bulk_recv.at[tile],
            device_id=across, device_id_type=MESH)

    @pl.loop(0, geo.n_tiles)
    def _(tile):
        part[tile] = jnp.zeros((TM, TN), F32)

        @pl.loop(0, n_chunk)
        def _(k):
            chunk = tile * n_chunk + k
            slot = lax.rem(chunk, NB)
            load_done(slot)
            later = chunk + (NB - 1)

            @pl.when(later < total_chunks)
            def _():
                load(lax.div(later, n_chunk), lax.rem(later, n_chunk), lax.rem(later, NB))

            part[tile] += lax.dot_general(
                xbuf[slot], ybuf[slot], (((0,), (0,)), ((), ())), preferred_element_type=F32)

        @pl.when(tile == 0)
        def _():
            pl.semaphore_wait(barrier, plane)
            for copy in w_copies:
                copy.start()

        bulk(tile).start()

    for copy in w_copies:
        copy.wait()

    beta_two, rho_step, clip_thr = hyper[0], hyper[1], hyper[2]

    for i in range(4):
        first, count, m_loc, n_loc = geo.mats[i]
        wide = m_loc == TM
        one, two = msg_one[i], msg_two
        w_out = w_outs[i]
        w_at = (lambda t, r: (pl.ds(r, RB), pl.ds(t * TN, TN))) if wide else (lambda t, r: (pl.ds(t * TM + r, RB), pl.ds(0, TN)))
        stat_at = (lambda t, r: pl.ds(r, RB)) if wide else (lambda t, r: pl.ds(t * TM + r, RB))
        col_at = m_loc

        if wide:
            rowpart[pl.ds(0, TM), :] = jnp.zeros((TM, LANES), F32)
        w_sq = jnp.zeros((8, LANES), F32)
        col_sum = jnp.zeros((8, TN), F32)
        for t in range(count):
            bulk(first + t).wait_recv()

            def stat_pass(b, carry):
                c_acc, w_acc = carry
                r = pl.multiple_of(b * RB, RB)
                grad = part[first + t, pl.ds(r, RB), :] + peer[first + t, pl.ds(r, RB), :]
                peer[first + t, pl.ds(r, RB), :] = grad
                sq = grad * grad + EPS_ONE
                folded = fold_lanes(sq)
                at = stat_at(t, r)
                if wide:
                    rowpart[at, :] += folded
                else:
                    rowpart[at, :] = folded
                w = w_out[w_at(t, r)]
                return c_acc + fold_rows(sq), w_acc + fold_rows(fold_lanes(w * w))

            col_sum, w_sq = lax.fori_loop(0, TM // RB, stat_pass, (col_sum, w_sq))
            if wide:
                one[pl.ds(me, 1), :, pl.ds(col_at + t * TN, TN)] = jnp.sum(col_sum, axis=0, keepdims=True)[None]
                col_sum = jnp.zeros((8, TN), F32)
        if not wide:
            one[pl.ds(me, 1), :, pl.ds(col_at, TN)] = jnp.sum(col_sum, axis=0, keepdims=True)[None]
        r_fold = jnp.zeros((1, LANES), F32)
        for j in range(0, m_loc, LANES):
            turned = jnp.transpose(rowpart[pl.ds(j, LANES), :])
            one[pl.ds(me, 1), :, pl.ds(j, LANES)] = jnp.sum(turned, axis=0, keepdims=True)[None]
            r_fold = r_fold + r_refs[i][:, pl.ds(j, LANES)]
        tail = m_loc + n_loc
        one[pl.ds(me, 1), :, pl.ds(tail, LANES)] = r_fold[None]
        one[pl.ds(me, 1), :, pl.ds(tail + LANES, LANES)] = jnp.sum(w_sq, axis=0, keepdims=True)[None]

        def exchange(buf, send, recv):
            copies = []
            for step in range(1, plane):
                _, device = plane_peer(step)
                copies.append(pltpu.make_async_remote_copy(
                    src_ref=buf.at[me], dst_ref=buf.at[me], send_sem=send.at[i, step], recv_sem=recv.at[i, me],
                    device_id=device, device_id_type=MESH))
            for copy in copies:
                copy.start()
            for step in range(1, plane):
                other, device = plane_peer(step)
                pltpu.make_async_remote_copy(
                    src_ref=buf.at[other], dst_ref=buf.at[other], send_sem=send.at[i, step], recv_sem=recv.at[i, other],
                    device_id=device, device_id_type=MESH).wait_recv()
            return copies

        sent = exchange(one, one_send, one_recv)

        m_total, n_total = m_loc * n_row, n_loc * n_col
        row_sum = one[row, :, pl.ds(0, m_loc)]
        for j in range(1, n_col):
            row_sum = row_sum + one[j * n_row + row, :, pl.ds(0, m_loc)]
        cols = [one[col * n_row + j, :, pl.ds(m_loc, n_loc)] for j in range(n_row)]
        while len(cols) > 1:
            cols = [cols[j] + cols[j + 1] for j in range(0, len(cols), 2)]
        new_row = beta_two * r_refs[i][...] + (1.0 - beta_two) * (row_sum / n_total)
        new_col = beta_two * c_refs[i][...] + (1.0 - beta_two) * (cols[0] / m_total)
        r_outs[i][...] = new_row
        c_outs[i][...] = new_col

        old_fold = jnp.zeros((1, LANES), F32)
        sq_fold = jnp.zeros((1, LANES), F32)
        w_fold = jnp.zeros((1, LANES), F32)
        for j in range(plane):
            sq_fold = sq_fold + fold_lanes(one[j, :, pl.ds(0, m_loc)])
            w_fold = w_fold + one[j, :, pl.ds(tail + LANES, LANES)]
            if j < n_row:
                old_fold = old_fold + one[j, :, pl.ds(tail, LANES)]
        row_total = jnp.sum(beta_two * old_fold + (1.0 - beta_two) * (sq_fold / n_total), axis=1, keepdims=True)
        w_rms = jnp.sqrt(jnp.sum(w_fold, axis=1, keepdims=True) / (m_total * n_total))

        row_scale = 1.0 / jnp.sqrt(new_row / row_total)
        col_scale = 1.0 / jnp.sqrt(new_col)
        for j in range(0, m_loc, LANES):
            spread = jnp.broadcast_to(row_scale[:, j:j + LANES], (LANES, LANES))
            acol[pl.ds(j, LANES), :] = jnp.transpose(spread)
        brow[:, pl.ds(0, n_loc)] = col_scale

        upd_sq = jnp.zeros((8, LANES), F32)
        for t in range(count):
            scale = brow[:, pl.ds(t * TN if wide else 0, TN)]

            def norm_pass(b, acc):
                r = pl.multiple_of(b * RB, RB)
                upd = peer[first + t, pl.ds(r, RB), :] * scale
                lane_scale = acol[stat_at(t, r), :]
                return acc + fold_rows(fold_lanes(upd * upd) * lane_scale * lane_scale)

            upd_sq = lax.fori_loop(0, TM // RB, norm_pass, upd_sq)
        two_i = two.at[i]
        two_i[pl.ds(me, 1)] = jnp.sum(upd_sq, axis=0, keepdims=True)[None]
        sent += exchange(two_i, two_send, two_recv)
        upd_fold = two_i[0]
        for j in range(1, plane):
            upd_fold = upd_fold + two_i[j]
        upd_rms = jnp.sqrt(jnp.sum(upd_fold, axis=1, keepdims=True) / (m_total * n_total))
        step_size = rho_step * jnp.maximum(EPS_TWO, w_rms) / jnp.maximum(1.0, upd_rms / clip_thr)
        brow[:, pl.ds(0, n_loc)] = col_scale * step_size
        for t in range(count):
            scale = brow[:, pl.ds(t * TN if wide else 0, TN)]

            def write_pass(b, _):
                r = pl.multiple_of(b * RB, RB)
                upd = peer[first + t, pl.ds(r, RB), :] * scale
                lane_scale = acol[stat_at(t, r), :]
                wide_scale = jnp.concatenate([lane_scale] * (TN // LANES), axis=1)
                w_out[w_at(t, r)] = w_out[w_at(t, r)] - upd * wide_scale
                return 0

            lax.fori_loop(0, TM // RB, write_pass, 0)
        for copy in sent:
            copy.wait_send()

    @pl.loop(0, geo.n_tiles)
    def _(tile):
        bulk(tile).wait_send()


class Geometry:
    def __init__(self, n_row, n_col, tokens, blocks):
        self.n_row, self.n_col = n_row, n_col
        self.n_chunk = tokens // KC
        self.mats, first = [], 0
        for m_loc, n_loc in blocks:
            count = (m_loc // TM) * (n_loc // TN)
            self.mats.append((first, count, m_loc, n_loc))
            first += count
        self.n_tiles = first

    def groups(self, x_refs, dy_refs):
        for (first, count, m_loc, _), x_ref, y_ref in zip(self.mats, x_refs, dy_refs):
            yield first, count, m_loc // TM, x_ref, y_ref


def solution(mesh):
    n_row, n_col = mesh.shape["row"], mesh.shape["col"]
    plane = n_row * n_col
    act_spec = P('dp', 'row')
    grad_spec = P('dp', 'col')
    w_spec = P('row', 'col')
    row_spec = P('row')
    col_spec = P('col')
    in_specs = (act_spec, grad_spec, act_spec, grad_spec, grad_spec, act_spec, grad_spec,
                w_spec, w_spec, w_spec, w_spec,
                row_spec, col_spec, row_spec, col_spec, row_spec, col_spec, row_spec, col_spec, P())
    out_specs = (w_spec, row_spec, col_spec) * 4

    def per_device(x_attn, dy_attn, x_mlp, dy_gate, dy_up, h_mlp, dy_out, w_attn, w_gate, w_up, w_down,
                   r_attn, c_attn, r_gate, c_gate, r_up, c_up, r_down, c_down, hyper_params):
        weights = (w_gate, w_up, w_down, w_attn)
        rows = [v.reshape(1, -1) for v in (r_gate, r_up, r_down, r_attn)]
        cols = [v.reshape(1, -1) for v in (c_gate, c_up, c_down, c_attn)]
        blocks = [w.shape for w in weights]
        geo = Geometry(n_row, n_col, x_attn.shape[0], blocks)
        hbm = pl.BlockSpec(memory_space=pl.ANY)
        vmem = pl.BlockSpec(memory_space=pltpu.VMEM)
        smem = pl.BlockSpec(memory_space=pltpu.SMEM)
        dma = pltpu.SemaphoreType.DMA
        max_m, max_n = max(b[0] for b in blocks), max(b[1] for b in blocks)

        def body(*refs):
            xs = (refs[0], refs[0], refs[1], refs[2])
            kernel(geo, xs, refs[3:7], refs[7:11], refs[11:15], refs[15:19], refs[19],
                   refs[20:24], refs[24:28], refs[28:32],
                   *refs[32:39], refs[39:43], *refs[43:])

        outs = pl.pallas_call(
            body,
            out_shape=tuple(pltpu.VMEM(w.shape, F32) for w in weights)
            + tuple(jax.ShapeDtypeStruct(v.shape, F32) for v in rows)
            + tuple(jax.ShapeDtypeStruct(v.shape, F32) for v in cols),
            in_specs=[hbm] * 3 + [hbm] * 4 + [hbm] * 4 + [vmem] * 8 + [smem],
            out_specs=(vmem,) * 12,
            scratch_shapes=[
                pltpu.VMEM((NB, KC, TM), jnp.bfloat16),
                pltpu.VMEM((NB, KC, TN), jnp.bfloat16),
                pltpu.VMEM((geo.n_tiles, TM, TN), F32),
                pltpu.VMEM((geo.n_tiles, TM, TN), F32),
                pltpu.VMEM((max_m, LANES), F32),
                pltpu.VMEM((max_m, LANES), F32),
                pltpu.VMEM((1, max_n), F32),
            ] + [pltpu.VMEM((plane, 1, m + n + 2 * LANES), F32) for m, n in blocks] + [
                pltpu.VMEM((4, plane, 1, LANES), F32),
                dma((NB,)), dma((NB,)), dma((4,)),
                dma((geo.n_tiles,)), dma((geo.n_tiles,)),
                dma((4, plane)), dma((4, plane)), dma((4, plane)), dma((4, plane)),
            ],
            compiler_params=pltpu.CompilerParams(
                collective_id=0, has_side_effects=True, vmem_limit_bytes=48 << 20),
            name="adafactor_step",
        )(x_mlp, h_mlp, x_attn, dy_gate, dy_up, dy_out, dy_attn, *weights, *rows, *cols, hyper_params)
        w_new, r_new, c_new = outs[:4], outs[4:8], outs[8:]
        result = []
        for i in (3, 0, 1, 2):
            result += [w_new[i], r_new[i].reshape(-1), c_new[i].reshape(-1)]
        return tuple(result)

    return jax.shard_map(per_device, mesh=mesh, in_specs=in_specs, out_specs=out_specs, check_vma=False)
```

```python
import functools
import math

import jax
import jax.numpy as jnp
from jax import lax
from jax.experimental import pallas as pl
from jax.experimental.pallas import tpu as pltpu
from jax.sharding import PartitionSpec as P

EPS_ONE = 1e-30
EPS_TWO = 1e-3
MESH = pl.DeviceIdType.MESH
F32 = jnp.float32

TM, TN = 256, 512
KC = 1024
NB = 8
RB = 32
LANES = 128


def fold_lanes(v):
    total = v[:, :LANES]
    for j in range(LANES, v.shape[1], LANES):
        total = total + v[:, j:j + LANES]
    return total


def fold_rows(v):
    total = v[:8]
    for i in range(8, v.shape[0], 8):
        total = total + v[i:i + 8]
    return total


def kernel(geo, x_refs, dy_refs, w_refs, r_refs, c_refs, hyper, w_outs, r_outs, c_outs,
           xbuf, ybuf, part, peer, rowpart, acol, brow, msg_one, msg_two,
           x_sem, y_sem, w_sem, bulk_send, bulk_recv, one_send, one_recv, two_send, two_recv):
    n_col, n_row, n_chunk = geo.n_col, geo.n_row, geo.n_chunk
    plane = n_col * n_row
    dp, col, row = lax.axis_index("dp"), lax.axis_index("col"), lax.axis_index("row")
    me = col * n_row + row

    def plane_peer(step):
        other = lax.rem(me + step, plane)
        return other, (dp, lax.div(other, n_row), lax.rem(other, n_row))

    across = (1 - dp, col, row)

    def load(tile, k, slot):
        rows = pl.ds(pl.multiple_of(k * KC, KC), KC)
        for first, count, m_tiles, x_ref, y_ref in geo.groups(x_refs, dy_refs):
            @pl.when(jnp.logical_and(tile >= first, tile < first + count))
            def _():
                local = tile - first
                m_at = local if m_tiles > 1 else 0
                n_at = 0 if m_tiles > 1 else local
                pltpu.make_async_copy(
                    x_ref.at[rows, pl.ds(pl.multiple_of(m_at * TM, TM), TM)], xbuf.at[slot], x_sem.at[slot]).start()
                pltpu.make_async_copy(
                    y_ref.at[rows, pl.ds(pl.multiple_of(n_at * TN, TN), TN)], ybuf.at[slot], y_sem.at[slot]).start()

    def load_done(slot):
        pltpu.make_async_copy(x_refs[0].at[pl.ds(0, KC), pl.ds(0, TM)], xbuf.at[slot], x_sem.at[slot]).wait()
        pltpu.make_async_copy(dy_refs[0].at[pl.ds(0, KC), pl.ds(0, TN)], ybuf.at[slot], y_sem.at[slot]).wait()

    total_chunks = geo.n_tiles * n_chunk
    for c in range(NB - 1):
        load(c // n_chunk, c % n_chunk, c)

    barrier = pltpu.get_barrier_semaphore()
    for step in range(1, plane):
        pl.semaphore_signal(barrier, inc=1, device_id=plane_peer(step)[1], device_id_type=MESH)
    pl.semaphore_signal(barrier, inc=1, device_id=across, device_id_type=MESH)
    w_copies = [pltpu.make_async_copy(w_refs[i], w_outs[i], w_sem.at[i]) for i in range(4)]

    def bulk(tile):
        return pltpu.make_async_remote_copy(
            src_ref=part.at[tile], dst_ref=peer.at[tile], send_sem=bulk_send.at[tile], recv_sem=bulk_recv.at[tile],
            device_id=across, device_id_type=MESH)

    @pl.loop(0, geo.n_tiles)
    def _(tile):
        part[tile] = jnp.zeros((TM, TN), F32)

        @pl.loop(0, n_chunk)
        def _(k):
            chunk = tile * n_chunk + k
            slot = lax.rem(chunk, NB)
            load_done(slot)
            later = chunk + (NB - 1)

            @pl.when(later < total_chunks)
            def _():
                load(lax.div(later, n_chunk), lax.rem(later, n_chunk), lax.rem(later, NB))

            part[tile] += lax.dot_general(
                xbuf[slot], ybuf[slot], (((0,), (0,)), ((), ())), preferred_element_type=F32)

        @pl.when(tile == 0)
        def _():
            pl.semaphore_wait(barrier, plane)
            for copy in w_copies:
                copy.start()

        bulk(tile).start()

    for copy in w_copies:
        copy.wait()

    beta_two, rho_step, clip_thr = hyper[0], hyper[1], hyper[2]

    for i in range(4):
        first, count, m_loc, n_loc = geo.mats[i]
        wide = m_loc == TM
        one, two = msg_one[i], msg_two
        w_out = w_outs[i]
        w_at = (lambda t, r: (pl.ds(r, RB), pl.ds(t * TN, TN))) if wide else (lambda t, r: (pl.ds(t * TM + r, RB), pl.ds(0, TN)))
        stat_at = (lambda t, r: pl.ds(r, RB)) if wide else (lambda t, r: pl.ds(t * TM + r, RB))
        col_at = m_loc

        if wide:
            rowpart[pl.ds(0, TM), :] = jnp.zeros((TM, LANES), F32)
        w_sq = jnp.zeros((8, LANES), F32)
        col_sum = jnp.zeros((8, TN), F32)
        for t in range(count):
            bulk(first + t).wait_recv()

            def stat_pass(b, carry):
                c_acc, w_acc = carry
                r = pl.multiple_of(b * RB, RB)
                grad = part[first + t, pl.ds(r, RB), :] + peer[first + t, pl.ds(r, RB), :]
                peer[first + t, pl.ds(r, RB), :] = grad
                sq = grad * grad + EPS_ONE
                folded = fold_lanes(sq)
                at = stat_at(t, r)
                if wide:
                    rowpart[at, :] += folded
                else:
                    rowpart[at, :] = folded
                w = w_out[w_at(t, r)]
                return c_acc + fold_rows(sq), w_acc + fold_rows(fold_lanes(w * w))

            col_sum, w_sq = lax.fori_loop(0, TM // RB, stat_pass, (col_sum, w_sq))
            if wide:
                one[pl.ds(me, 1), :, pl.ds(col_at + t * TN, TN)] = jnp.sum(col_sum, axis=0, keepdims=True)[None]
                col_sum = jnp.zeros((8, TN), F32)
        if not wide:
            one[pl.ds(me, 1), :, pl.ds(col_at, TN)] = jnp.sum(col_sum, axis=0, keepdims=True)[None]
        r_fold = jnp.zeros((1, LANES), F32)
        for j in range(0, m_loc, LANES):
            turned = jnp.transpose(rowpart[pl.ds(j, LANES), :])
            one[pl.ds(me, 1), :, pl.ds(j, LANES)] = jnp.sum(turned, axis=0, keepdims=True)[None]
            r_fold = r_fold + r_refs[i][:, pl.ds(j, LANES)]
        tail = m_loc + n_loc
        one[pl.ds(me, 1), :, pl.ds(tail, LANES)] = r_fold[None]
        one[pl.ds(me, 1), :, pl.ds(tail + LANES, LANES)] = jnp.sum(w_sq, axis=0, keepdims=True)[None]

        def exchange(buf, send, recv):
            copies = []
            for step in range(1, plane):
                _, device = plane_peer(step)
                copies.append(pltpu.make_async_remote_copy(
                    src_ref=buf.at[me], dst_ref=buf.at[me], send_sem=send.at[i, step], recv_sem=recv.at[i, me],
                    device_id=device, device_id_type=MESH))
            for copy in copies:
                copy.start()
            for step in range(1, plane):
                other, device = plane_peer(step)
                pltpu.make_async_remote_copy(
                    src_ref=buf.at[other], dst_ref=buf.at[other], send_sem=send.at[i, step], recv_sem=recv.at[i, other],
                    device_id=device, device_id_type=MESH).wait_recv()
            return copies

        sent = exchange(one, one_send, one_recv)

        m_total, n_total = m_loc * n_row, n_loc * n_col
        row_sum = one[row, :, pl.ds(0, m_loc)]
        for j in range(1, n_col):
            row_sum = row_sum + one[j * n_row + row, :, pl.ds(0, m_loc)]
        cols = [one[col * n_row + j, :, pl.ds(m_loc, n_loc)] for j in range(n_row)]
        while len(cols) > 1:
            cols = [cols[j] + cols[j + 1] for j in range(0, len(cols), 2)]
        new_row = beta_two * r_refs[i][...] + (1.0 - beta_two) * (row_sum / n_total)
        new_col = beta_two * c_refs[i][...] + (1.0 - beta_two) * (cols[0] / m_total)
        r_outs[i][...] = new_row
        c_outs[i][...] = new_col

        old_fold = jnp.zeros((1, LANES), F32)
        sq_fold = jnp.zeros((1, LANES), F32)
        w_fold = jnp.zeros((1, LANES), F32)
        for j in range(plane):
            sq_fold = sq_fold + fold_lanes(one[j, :, pl.ds(0, m_loc)])
            w_fold = w_fold + one[j, :, pl.ds(tail + LANES, LANES)]
            if j < n_row:
                old_fold = old_fold + one[j, :, pl.ds(tail, LANES)]
        row_total = jnp.sum(beta_two * old_fold + (1.0 - beta_two) * (sq_fold / n_total), axis=1, keepdims=True)
        w_rms = jnp.sqrt(jnp.sum(w_fold, axis=1, keepdims=True) / (m_total * n_total))

        row_scale = 1.0 / jnp.sqrt(new_row / row_total)
        col_scale = 1.0 / jnp.sqrt(new_col)
        for j in range(0, m_loc, LANES):
            spread = jnp.broadcast_to(row_scale[:, j:j + LANES], (LANES, LANES))
            acol[pl.ds(j, LANES), :] = jnp.transpose(spread)
        brow[:, pl.ds(0, n_loc)] = col_scale

        upd_sq = jnp.zeros((8, LANES), F32)
        for t in range(count):
            scale = brow[:, pl.ds(t * TN if wide else 0, TN)]

            def norm_pass(b, acc):
                r = pl.multiple_of(b * RB, RB)
                upd = peer[first + t, pl.ds(r, RB), :] * scale
                lane_scale = acol[stat_at(t, r), :]
                return acc + fold_rows(fold_lanes(upd * upd) * lane_scale * lane_scale)

            upd_sq = lax.fori_loop(0, TM // RB, norm_pass, upd_sq)
        two_i = two.at[i]
        two_i[pl.ds(me, 1)] = jnp.sum(upd_sq, axis=0, keepdims=True)[None]
        sent += exchange(two_i, two_send, two_recv)
        upd_fold = two_i[0]
        for j in range(1, plane):
            upd_fold = upd_fold + two_i[j]
        upd_rms = jnp.sqrt(jnp.sum(upd_fold, axis=1, keepdims=True) / (m_total * n_total))
        step_size = rho_step * jnp.maximum(EPS_TWO, w_rms) / jnp.maximum(1.0, upd_rms / clip_thr)
        brow[:, pl.ds(0, n_loc)] = col_scale * step_size
        for t in range(count):
            scale = brow[:, pl.ds(t * TN if wide else 0, TN)]

            def write_pass(b, _):
                r = pl.multiple_of(b * RB, RB)
                upd = peer[first + t, pl.ds(r, RB), :] * scale
                lane_scale = acol[stat_at(t, r), :]
                wide_scale = jnp.concatenate([lane_scale] * (TN // LANES), axis=1)
                w_out[w_at(t, r)] = w_out[w_at(t, r)] - upd * wide_scale
                return 0

            lax.fori_loop(0, TM // RB, write_pass, 0)
        for copy in sent:
            copy.wait_send()

    @pl.loop(0, geo.n_tiles)
    def _(tile):
        bulk(tile).wait_send()


def write_out(*refs):
    copies = [pltpu.make_async_copy(refs[i], refs[12 + i], refs[24].at[i]) for i in range(12)]
    for copy in copies:
        copy.start()
    for copy in copies:
        copy.wait()


class Geometry:
    def __init__(self, n_row, n_col, tokens, blocks):
        self.n_row, self.n_col = n_row, n_col
        self.n_chunk = tokens // KC
        self.mats, first = [], 0
        for m_loc, n_loc in blocks:
            count = (m_loc // TM) * (n_loc // TN)
            self.mats.append((first, count, m_loc, n_loc))
            first += count
        self.n_tiles = first

    def groups(self, x_refs, dy_refs):
        for (first, count, m_loc, _), x_ref, y_ref in zip(self.mats, x_refs, dy_refs):
            yield first, count, m_loc // TM, x_ref, y_ref


def solution(mesh):
    n_row, n_col = mesh.shape["row"], mesh.shape["col"]
    plane = n_row * n_col
    act_spec = P('dp', 'row')
    grad_spec = P('dp', 'col')
    w_spec = P('row', 'col')
    row_spec = P('row')
    col_spec = P('col')
    in_specs = (act_spec, grad_spec, act_spec, grad_spec, grad_spec, act_spec, grad_spec,
                w_spec, w_spec, w_spec, w_spec,
                row_spec, col_spec, row_spec, col_spec, row_spec, col_spec, row_spec, col_spec, P())
    out_specs = (w_spec, row_spec, col_spec) * 4

    def per_device(x_attn, dy_attn, x_mlp, dy_gate, dy_up, h_mlp, dy_out, w_attn, w_gate, w_up, w_down,
                   r_attn, c_attn, r_gate, c_gate, r_up, c_up, r_down, c_down, hyper_params):
        weights = (w_gate, w_up, w_down, w_attn)
        rows = [v.reshape(1, -1) for v in (r_gate, r_up, r_down, r_attn)]
        cols = [v.reshape(1, -1) for v in (c_gate, c_up, c_down, c_attn)]
        blocks = [w.shape for w in weights]
        geo = Geometry(n_row, n_col, x_attn.shape[0], blocks)
        results = (*weights, *rows, *cols)
        hbm = pl.BlockSpec(memory_space=pl.ANY)
        vmem = pl.BlockSpec(memory_space=pltpu.VMEM)
        smem = pl.BlockSpec(memory_space=pltpu.SMEM)
        dma = pltpu.SemaphoreType.DMA
        max_m, max_n = max(b[0] for b in blocks), max(b[1] for b in blocks)

        def body(*refs):
            xs = (refs[0], refs[0], refs[1], refs[2])
            kernel(geo, xs, refs[3:7], refs[7:11], refs[11:15], refs[15:19], refs[19],
                   refs[20:24], refs[24:28], refs[28:32],
                   *refs[32:39], refs[39:43], *refs[43:])

        outs = pl.pallas_call(
            body,
            out_shape=tuple(pltpu.VMEM(v.shape, F32) for v in results),
            in_specs=[hbm] * 3 + [hbm] * 4 + [hbm] * 4 + [vmem] * 8 + [smem],
            out_specs=(vmem,) * 12,
            scratch_shapes=[
                pltpu.VMEM((NB, KC, TM), jnp.bfloat16),
                pltpu.VMEM((NB, KC, TN), jnp.bfloat16),
                pltpu.VMEM((geo.n_tiles, TM, TN), F32),
                pltpu.VMEM((geo.n_tiles, TM, TN), F32),
                pltpu.VMEM((max_m, LANES), F32),
                pltpu.VMEM((max_m, LANES), F32),
                pltpu.VMEM((1, max_n), F32),
            ] + [pltpu.VMEM((plane, 1, m + n + 2 * LANES), F32) for m, n in blocks] + [
                pltpu.VMEM((4, plane, 1, LANES), F32),
                dma((NB,)), dma((NB,)), dma((4,)),
                dma((geo.n_tiles,)), dma((geo.n_tiles,)),
                dma((4, plane)), dma((4, plane)), dma((4, plane)), dma((4, plane)),
            ],
            compiler_params=pltpu.CompilerParams(
                collective_id=0, has_side_effects=True, vmem_limit_bytes=48 << 20),
            name="adafactor_step",
        )(x_mlp, h_mlp, x_attn, dy_gate, dy_up, dy_out, dy_attn, *weights, *rows, *cols, hyper_params)
        outs = pl.pallas_call(
            write_out,
            out_shape=tuple(jax.ShapeDtypeStruct(v.shape, F32) for v in results),
            in_specs=[vmem] * 12,
            out_specs=(hbm,) * 12,
            scratch_shapes=[dma((12,))],
            name="write_out", compiler_params=pltpu.CompilerParams(vmem_limit_bytes=1 << 20),
        )(*[pltpu.with_memory_space_constraint(v, pltpu.VMEM) for v in outs])
        w_new, r_new, c_new = outs[:4], outs[4:8], outs[8:]
        result = []
        for i in (3, 0, 1, 2):
            result += [w_new[i], r_new[i].reshape(-1), c_new[i].reshape(-1)]
        return tuple(result)

    return jax.shard_map(per_device, mesh=mesh, in_specs=in_specs, out_specs=out_specs, check_vma=False)
```

```python
import jax
import jax.numpy as jnp
from jax import lax
from jax.experimental import pallas as pl
from jax.experimental.pallas import tpu as pltpu
from jax.sharding import PartitionSpec as P

EPS_ONE = 1e-30
EPS_TWO = 1e-3
MESH = pl.DeviceIdType.MESH
F32 = jnp.float32

TM, TN = 256, 512
HALVES = 2
PARTS = ((0, 128, 0, 128), (128, 128, 0, 128), (0, 256, 128, 128), (0, 256, 256, 256))
RB = 32
LANES = 128


def fold_lanes(v):
    total = v[:, :LANES]
    for j in range(LANES, v.shape[1], LANES):
        total = total + v[:, j:j + LANES]
    return total


def fold_rows(v):
    total = v[:8]
    for i in range(8, v.shape[0], 8):
        total = total + v[i:i + 8]
    return total


def lane_sum(v):
    return jnp.sum(v, axis=1, keepdims=True)


def row_sum_of(v):
    return jnp.sum(v, axis=0, keepdims=True)


def kernel(geo, x_refs, dy_refs, w_refs, r_refs, c_refs, hyper, w_outs, r_outs, c_outs,
           xbuf, ybuf, part, peer, rowpart, rowpart_own, acol, brow, colpart, w_sq, msg_one, msg_two, zmsg_one, zmsg_two,
           x_sem, y_sem, first_sem, w_sem, sub_send, sub_recv, bulk_send, bulk_recv, gather_sem,
           one_send, one_recv, two_send, two_recv, z_send, z_recv):
    n_col, n_row = geo.n_col, geo.n_row
    plane = n_col * n_row
    dp, col, row = lax.axis_index("dp"), lax.axis_index("col"), lax.axis_index("row")
    me = col * n_row + row
    own, other = dp, 1 - dp
    across = (1 - dp, col, row)

    def plane_peer(step):
        other = lax.rem(me + step, plane)
        return other, (dp, lax.div(other, n_row), lax.rem(other, n_row))

    def remote(src, dst, send, recv, device):
        return pltpu.make_async_remote_copy(
            src_ref=src, dst_ref=dst, send_sem=send, recv_sem=recv, device_id=device, device_id_type=MESH)

    def first_part(tile, j):
        r0, r_n, c0, c_n = PARTS[j]
        at = (tile, pl.ds(r0, r_n), pl.ds(c0, c_n))
        return remote(part.at[at], peer.at[at], sub_send.at[j], sub_recv.at[j], across)

    def bulk(tile):
        return remote(part.at[tile], peer.at[tile], bulk_send.at[tile], bulk_recv.at[tile], across)

    def gather(tile):
        at = (slice(None), pl.ds(pl.multiple_of(tile * TN, TN), TN))
        return remote(w_outs[0].at[at], w_outs[0].at[at], gather_sem.at[0], gather_sem.at[1], across)

    def z_copy(n, buf, slot):
        return remote(buf.at[slot], buf.at[slot], z_send.at[n], z_recv.at[n], across)

    half = geo.tokens // HALVES

    def first_x(n, pieces, c, c0, c_n):
        rows = pl.ds(c * (geo.tokens // pieces), geo.tokens // pieces)
        at = (rows, pl.ds(c0, c_n))
        return pltpu.make_async_copy(x_refs[0].at[at], xbuf.at[0].at[at], first_sem.at[n, c])

    def first_y(n, pieces, c, c0, c_n):
        rows = pl.ds(c * (geo.tokens // pieces), geo.tokens // pieces)
        columns = pl.ds(pl.multiple_of(other * TN + c0, LANES), c_n)
        return pltpu.make_async_copy(dy_refs[0].at[rows, columns], ybuf.at[0, rows, pl.ds(c0, c_n)], first_sem.at[n, c])

    n_steps = geo.n_tiles - 1

    def tile_of(s):
        past_zero = lax.div(s + (n_steps - 1), n_steps)
        past_one = lax.div(s + (n_steps - 2), n_steps)
        return s + 1 + (1 - past_zero) - (past_zero - past_one) * (2 - own)

    def slot_of(s):
        return lax.rem(s + 1, 2)

    def load(s):
        tile, slot = tile_of(s), slot_of(s)
        for first, count, m_tiles, x_ref, y_ref in geo.groups(x_refs, dy_refs):
            @pl.when(jnp.logical_and(tile >= first, tile < first + count))
            def _():
                local = tile - first
                m_at = local if m_tiles > 1 else 0
                n_at = 0 if m_tiles > 1 else local
                for h in range(HALVES):
                    rows = pl.ds(h * half, half)
                    pltpu.make_async_copy(
                        x_ref.at[rows, pl.ds(pl.multiple_of(m_at * TM, TM), TM)],
                        xbuf.at[slot, rows], x_sem.at[slot, h]).start()
                    pltpu.make_async_copy(
                        y_ref.at[rows, pl.ds(pl.multiple_of(n_at * TN, TN), TN)],
                        ybuf.at[slot, rows], y_sem.at[slot, h]).start()

    def load_done(slot, h):
        rows = pl.ds(h * half, half)
        pltpu.make_async_copy(x_refs[0].at[rows, pl.ds(0, TM)], xbuf.at[slot, rows], x_sem.at[slot, h]).wait()
        pltpu.make_async_copy(dy_refs[0].at[rows, pl.ds(0, TN)], ybuf.at[slot, rows], y_sem.at[slot, h]).wait()

    def contract(x, y):
        return lax.dot_general(x, y, (((0,), (0,)), ((), ())), preferred_element_type=F32)

    first_loads = (
        (4, lambda c: (first_x(0, 4, c, 0, 128), first_y(1, 4, c, 0, 128))),
        (2, lambda c: (first_x(2, 2, c, 128, 128),)),
        (2, lambda c: (first_y(3, 2, c, 128, 128),)),
        (2, lambda c: (first_y(4, 2, c, 256, 256),)),
    )
    for pieces, copies_of in first_loads:
        for c in range(pieces):
            for copy in copies_of(c):
                copy.start()
    load(0)

    barrier = pltpu.get_barrier_semaphore()
    for step in range(1, plane):
        pl.semaphore_signal(barrier, inc=1, device_id=plane_peer(step)[1], device_id_type=MESH)
    pl.semaphore_signal(barrier, inc=1, device_id=across, device_id_type=MESH)

    for j, (pieces, copies_of) in enumerate(first_loads):
        r0, r_n, c0, c_n = PARTS[j]
        at = (other, pl.ds(r0, r_n), pl.ds(c0, c_n))
        for c in range(pieces):
            for copy in copies_of(c):
                copy.wait()
            rows = pl.ds(c * (geo.tokens // pieces), geo.tokens // pieces)
            term = contract(xbuf[0, rows, pl.ds(r0, r_n)], ybuf[0, rows, pl.ds(c0, c_n)])
            part[at] = term if c == 0 else part[at] + term
        if j == 0:
            pl.semaphore_wait(barrier, plane)
        first_part(other, j).start()
    w_copies = [pltpu.make_async_copy(w_refs[i], w_outs[i], w_sem.at[i]) for i in range(4)]

    def tiles(lo, hi):
        @pl.loop(lo, hi)
        def _(s):
            tile, slot = tile_of(s), slot_of(s)

            @pl.when(s + 1 < n_steps)
            def _():
                load(s + 1)

            for h in range(HALVES):
                load_done(slot, h)
                rows = pl.ds(h * half, half)
                term = contract(xbuf[slot, rows, :], ybuf[slot, rows, :])
                if h == 0:
                    part[tile] = term
                else:
                    part[tile] += term

            @pl.when(s != 1)
            def _():
                bulk(tile).start()

    beta_two, rho_step, clip_thr = hyper[0], hyper[1], hyper[2]

    def w_at(i, t, r):
        if geo.wide(i):
            return pl.ds(r, RB), pl.ds(pl.multiple_of(t * TN, TN), TN)
        return pl.ds(t * TM + r, RB), pl.ds(0, TN)

    def stat_at(i, t, r):
        return pl.ds(r, RB) if geo.wide(i) else pl.ds(t * TM + r, RB)

    def stat_tile(i, t, rows_ref, accumulate, col_sum):
        tile = geo.mats[i][0] + t

        def step(b, acc):
            r = pl.multiple_of(b * RB, RB)
            grad = part[tile, pl.ds(r, RB), :] + peer[tile, pl.ds(r, RB), :]
            peer[tile, pl.ds(r, RB), :] = grad
            sq = grad * grad + EPS_ONE
            at = stat_at(i, t, r)
            if accumulate:
                rows_ref[at, :] += fold_lanes(sq)
            else:
                rows_ref[at, :] = fold_lanes(sq)
            return acc + fold_rows(sq)

        return lax.fori_loop(0, TM // RB, step, col_sum)

    def norm_tile(i, t, acc):
        tile = geo.mats[i][0] + t
        scale = brow[:, pl.ds(pl.multiple_of(t * TN, TN), TN)] if geo.wide(i) else brow[:, pl.ds(0, TN)]

        def step(b, acc):
            r = pl.multiple_of(b * RB, RB)
            upd = peer[tile, pl.ds(r, RB), :] * scale
            lane_scale = acol[stat_at(i, t, r), :]
            return acc + fold_rows(fold_lanes(upd * upd) * lane_scale * lane_scale)

        return lax.fori_loop(0, TM // RB, step, acc)

    def write_tile(i, t, step_size):
        tile = geo.mats[i][0] + t
        scale = brow[:, pl.ds(pl.multiple_of(t * TN, TN), TN)] if geo.wide(i) else brow[:, pl.ds(0, TN)]
        scale = scale * step_size

        def step(b, _):
            r = pl.multiple_of(b * RB, RB)
            upd = peer[tile, pl.ds(r, RB), :] * scale
            lane_scale = jnp.concatenate([acol[stat_at(i, t, r), :]] * (TN // LANES), axis=1)
            w_outs[i][w_at(i, t, r)] = w_outs[i][w_at(i, t, r)] - upd * lane_scale
            return 0

        lax.fori_loop(0, TM // RB, step, 0)

    def weight_squares(i):
        acc = jnp.zeros((8, LANES), F32)
        for t in range(geo.mats[i][1]):
            def step(b, acc):
                w = w_outs[i][w_at(i, t, pl.multiple_of(b * RB, RB))]
                return acc + fold_rows(fold_lanes(w * w))

            acc = lax.fori_loop(0, TM // RB, step, acc)
        w_sq[pl.ds(i, 1), :] = row_sum_of(acc)

    def row_totals(rows_ref, j):
        return row_sum_of(jnp.transpose(rows_ref[pl.ds(j, LANES), :]))

    def exchange(i, buf, send, recv):
        copies = []
        for step in range(1, plane):
            device = plane_peer(step)[1]
            copies.append(remote(buf.at[me], buf.at[me], send.at[i, step], recv.at[i, me], device))
        for copy in copies:
            copy.start()
        for step in range(1, plane):
            there, device = plane_peer(step)
            remote(buf.at[there], buf.at[there], send.at[i, step], recv.at[i, there], device).wait_recv()
        return copies

    def sizes(i):
        _, _, m_loc, n_loc = geo.mats[i]
        return m_loc, n_loc, m_loc + n_loc, m_loc * n_row, n_loc * n_col

    def round_one(i, z_part):
        m_loc, n_loc, tail, m_total, n_total = sizes(i)
        one = msg_one[i]
        r_fold = jnp.zeros((1, LANES), F32)
        for j in range(0, m_loc, LANES):
            total = row_totals(rowpart, j)
            if z_part:
                total = total + (zmsg_one[0, :, pl.ds(j, LANES)] + zmsg_one[1, :, pl.ds(j, LANES)])
            one[pl.ds(me, 1), :, pl.ds(j, LANES)] = total[None]
            r_fold = r_fold + r_refs[i][:, pl.ds(j, LANES)]
        one[pl.ds(me, 1), :, pl.ds(m_loc, n_loc)] = colpart[:, pl.ds(0, n_loc)][None]
        if z_part:
            for t in range(2):
                one[pl.ds(me, 1), :, pl.ds(m_loc + t * TN, TN)] = zmsg_one[t, :, pl.ds(m_loc, TN)][None]
        one[pl.ds(me, 1), :, pl.ds(tail, LANES)] = r_fold[None]
        one[pl.ds(me, 1), :, pl.ds(tail + LANES, LANES)] = w_sq[pl.ds(i, 1), :][None]
        sent = exchange(i, one, one_send, one_recv)

        row_sum = one[row, :, pl.ds(0, m_loc)]
        for j in range(1, n_col):
            row_sum = row_sum + one[j * n_row + row, :, pl.ds(0, m_loc)]
        col_sum = one[col * n_row, :, pl.ds(m_loc, n_loc)]
        for j in range(1, n_row):
            col_sum = col_sum + one[col * n_row + j, :, pl.ds(m_loc, n_loc)]
        new_row = beta_two * r_refs[i][...] + (1.0 - beta_two) * (row_sum / n_total)
        new_col = beta_two * c_refs[i][...] + (1.0 - beta_two) * (col_sum / m_total)
        r_outs[i][...] = new_row
        c_outs[i][...] = new_col

        old_fold = jnp.zeros((1, LANES), F32)
        sq_fold = jnp.zeros((1, LANES), F32)
        for j in range(plane):
            sq_fold = sq_fold + fold_lanes(one[j, :, pl.ds(0, m_loc)])
            if j < n_row:
                old_fold = old_fold + one[j, :, pl.ds(tail, LANES)]
        total = lane_sum(beta_two * old_fold + (1.0 - beta_two) * (sq_fold / n_total))

        row_scale = 1.0 / jnp.sqrt(new_row / total)
        for j in range(0, m_loc, LANES):
            acol[pl.ds(j, LANES), :] = jnp.transpose(jnp.broadcast_to(row_scale[:, j:j + LANES], (LANES, LANES)))
        brow[:, pl.ds(0, n_loc)] = 1.0 / jnp.sqrt(new_col)
        return sent

    def round_two(i, upd_sq):
        _, _, tail, m_total, n_total = sizes(i)
        one, two = msg_one[i], msg_two.at[i]
        two[pl.ds(me, 1)] = upd_sq[None]
        sent = exchange(i, two, two_send, two_recv)
        upd_fold, w_fold = two[0], one[0, :, pl.ds(tail + LANES, LANES)]
        for j in range(1, plane):
            upd_fold = upd_fold + two[j]
            w_fold = w_fold + one[j, :, pl.ds(tail + LANES, LANES)]
        upd_rms = jnp.sqrt(lane_sum(upd_fold) / (m_total * n_total))
        w_rms = jnp.sqrt(lane_sum(w_fold) / (m_total * n_total))
        return rho_step * jnp.maximum(EPS_TWO, w_rms) / jnp.maximum(1.0, upd_rms / clip_thr), sent

    none = jnp.zeros((8, TN), F32)
    no_lanes = jnp.zeros((8, LANES), F32)
    m_gate = geo.mats[0][2]

    tiles(0, 4)

    for copy in w_copies:
        copy.start()
    for copy in w_copies:
        copy.wait()
    for i in range(4):
        weight_squares(i)
    for j in range(len(PARTS)):
        first_part(own, j).wait_recv()
    own_col = stat_tile(0, own, rowpart_own, False, none)
    for j in range(0, TM, LANES):
        zmsg_one[pl.ds(own, 1), :, pl.ds(j, LANES)] = row_totals(rowpart_own, j)[None]
    zmsg_one[pl.ds(own, 1), :, pl.ds(m_gate, TN)] = row_sum_of(own_col)[None]
    z_copy(0, zmsg_one, own).start()

    tiles(4, 6)

    shared = range(2, geo.mats[0][1])
    for t in shared:
        bulk(t).wait_recv()
        colpart[:, pl.ds(t * TN, TN)] = row_sum_of(stat_tile(0, t, rowpart, t > 2, none))
    z_copy(0, zmsg_one, other).wait_recv()
    gate_sent = round_one(0, True)
    zmsg_two[pl.ds(own, 1)] = row_sum_of(norm_tile(0, own, no_lanes))[None]
    z_copy(1, zmsg_two, own).start()

    tiles(6, 8)

    upd_sq = no_lanes
    for t in shared:
        upd_sq = norm_tile(0, t, upd_sq)
    z_copy(1, zmsg_two, other).wait_recv()
    step_size, sent = round_two(0, row_sum_of(upd_sq) + (zmsg_two[0] + zmsg_two[1]))
    gate_sent += sent
    write_tile(0, own, step_size)
    for t in shared:
        write_tile(0, t, step_size)

    tiles(8, geo.n_tiles - 1)
    gather(own).start()

    for i in range(1, 4):
        first, count, m_loc, n_loc = geo.mats[i]
        col_sum = none
        for t in range(count):
            bulk(first + t).wait_recv()
            if geo.wide(i):
                colpart[:, pl.ds(t * TN, TN)] = row_sum_of(stat_tile(i, t, rowpart, t > 0, none))
            else:
                col_sum = stat_tile(i, t, rowpart, False, col_sum)
        if not geo.wide(i):
            colpart[:, pl.ds(0, TN)] = row_sum_of(col_sum)
        sent_one = round_one(i, False)
        upd_sq = no_lanes
        for t in range(count):
            upd_sq = norm_tile(i, t, upd_sq)
        step_size, sent_two = round_two(i, row_sum_of(upd_sq))
        for t in range(count):
            write_tile(i, t, step_size)
        for copy in sent_one + sent_two:
            copy.wait_send()

    for copy in gate_sent:
        copy.wait_send()
    z_copy(0, zmsg_one, own).wait_send()
    z_copy(1, zmsg_two, own).wait_send()
    for j in range(len(PARTS)):
        first_part(other, j).wait_send()

    @pl.loop(2, geo.n_tiles)
    def _(tile):
        bulk(tile).wait_send()

    gather(own).wait_send()
    gather(other).wait_recv()


def write_out(*refs):
    copies = [pltpu.make_async_copy(refs[i], refs[12 + i], refs[24].at[i]) for i in range(12)]
    for copy in copies:
        copy.start()
    for copy in copies:
        copy.wait()


class Geometry:
    def __init__(self, n_row, n_col, tokens, blocks):
        self.n_row, self.n_col = n_row, n_col
        self.tokens = tokens
        self.mats, first = [], 0
        for m_loc, n_loc in blocks:
            count = (m_loc // TM) * (n_loc // TN)
            self.mats.append((first, count, m_loc, n_loc))
            first += count
        self.n_tiles = first

    def wide(self, i):
        return self.mats[i][2] == TM

    def groups(self, x_refs, dy_refs):
        for (first, count, m_loc, _), x_ref, y_ref in zip(self.mats, x_refs, dy_refs):
            yield first, count, m_loc // TM, x_ref, y_ref


def solution(mesh):
    n_row, n_col = mesh.shape["row"], mesh.shape["col"]
    plane = n_row * n_col
    act_spec = P('dp', 'row')
    grad_spec = P('dp', 'col')
    w_spec = P('row', 'col')
    row_spec = P('row')
    col_spec = P('col')
    in_specs = (act_spec, grad_spec, act_spec, grad_spec, grad_spec, act_spec, grad_spec,
                w_spec, w_spec, w_spec, w_spec,
                row_spec, col_spec, row_spec, col_spec, row_spec, col_spec, row_spec, col_spec, P())
    out_specs = (w_spec, row_spec, col_spec) * 4

    def per_device(x_attn, dy_attn, x_mlp, dy_gate, dy_up, h_mlp, dy_out, w_attn, w_gate, w_up, w_down,
                   r_attn, c_attn, r_gate, c_gate, r_up, c_up, r_down, c_down, hyper_params):
        weights = (w_gate, w_up, w_down, w_attn)
        rows = [v.reshape(1, -1) for v in (r_gate, r_up, r_down, r_attn)]
        cols = [v.reshape(1, -1) for v in (c_gate, c_up, c_down, c_attn)]
        blocks = [w.shape for w in weights]
        geo = Geometry(n_row, n_col, x_attn.shape[0], blocks)
        results = (*weights, *rows, *cols)
        hbm = pl.BlockSpec(memory_space=pl.ANY)
        vmem = pl.BlockSpec(memory_space=pltpu.VMEM)
        smem = pl.BlockSpec(memory_space=pltpu.SMEM)
        dma = pltpu.SemaphoreType.DMA
        max_m, max_n = max(b[0] for b in blocks), max(b[1] for b in blocks)

        def body(*refs):
            xs = (refs[0], refs[0], refs[1], refs[2])
            kernel(geo, xs, refs[3:7], refs[7:11], refs[11:15], refs[15:19], refs[19],
                   refs[20:24], refs[24:28], refs[28:32],
                   *refs[32:42], refs[42:46], *refs[46:])

        outs = pl.pallas_call(
            body,
            out_shape=tuple(pltpu.VMEM(v.shape, F32) for v in results),
            in_specs=[hbm] * 11 + [vmem] * 8 + [smem],
            out_specs=(vmem,) * 12,
            scratch_shapes=[
                pltpu.VMEM((2, geo.tokens, TM), jnp.bfloat16),
                pltpu.VMEM((2, geo.tokens, TN), jnp.bfloat16),
                pltpu.VMEM((geo.n_tiles, TM, TN), F32),
                pltpu.VMEM((geo.n_tiles, TM, TN), F32),
                pltpu.VMEM((max_m, LANES), F32),
                pltpu.VMEM((TM, LANES), F32),
                pltpu.VMEM((max_m, LANES), F32),
                pltpu.VMEM((1, max_n), F32),
                pltpu.VMEM((1, max_n), F32),
                pltpu.VMEM((8, LANES), F32),
            ] + [pltpu.VMEM((plane, 1, m + n + 2 * LANES), F32) for m, n in blocks] + [
                pltpu.VMEM((4, plane, 1, LANES), F32),
                pltpu.VMEM((2, 1, TM + TN), F32),
                pltpu.VMEM((2, 1, LANES), F32),
                dma((2, HALVES)), dma((2, HALVES)), dma((5, 4)), dma((4,)),
                dma((len(PARTS),)), dma((len(PARTS),)), dma((geo.n_tiles,)), dma((geo.n_tiles,)), dma((2,)),
                dma((4, plane)), dma((4, plane)), dma((4, plane)), dma((4, plane)), dma((2,)), dma((2,)),
            ],
            compiler_params=pltpu.CompilerParams(
                collective_id=0, has_side_effects=True, vmem_limit_bytes=48 << 20),
            name="adafactor_step",
        )(x_mlp, h_mlp, x_attn, dy_gate, dy_up, dy_out, dy_attn, *weights, *rows, *cols, hyper_params)
        outs = pl.pallas_call(
            write_out,
            out_shape=tuple(jax.ShapeDtypeStruct(v.shape, F32) for v in results),
            in_specs=[vmem] * 12,
            out_specs=(hbm,) * 12,
            scratch_shapes=[dma((12,))],
            compiler_params=pltpu.CompilerParams(vmem_limit_bytes=1 << 20),
            name="write_out",
        )(*[pltpu.with_memory_space_constraint(v, pltpu.VMEM) for v in outs])
        w_new, r_new, c_new = outs[:4], outs[4:8], outs[8:]
        result = []
        for i in (3, 0, 1, 2):
            result += [w_new[i], r_new[i].reshape(-1), c_new[i].reshape(-1)]
        return tuple(result)

    return jax.shard_map(per_device, mesh=mesh, in_specs=in_specs, out_specs=out_specs, check_vma=False)
```

```python
import jax
import jax.numpy as jnp
from jax import lax
from jax.experimental import pallas as pl
from jax.experimental.pallas import tpu as pltpu
from jax.sharding import PartitionSpec as P

EPS_ONE = 1e-30
EPS_TWO = 1e-3
MESH = pl.DeviceIdType.MESH
F32 = jnp.float32

TM, TN = 256, 512
HALVES = 2
PARTS = ((0, 128, 0, 128), (128, 128, 0, 128), (0, 256, 128, 128), (0, 256, 256, 256))
RB = 32
LANES = 128


def fold_lanes(v):
    total = v[:, :LANES]
    for j in range(LANES, v.shape[1], LANES):
        total = total + v[:, j:j + LANES]
    return total


def fold_rows(v):
    total = v[:8]
    for i in range(8, v.shape[0], 8):
        total = total + v[i:i + 8]
    return total


def lane_sum(v):
    return jnp.sum(v, axis=1, keepdims=True)


def row_sum_of(v):
    return jnp.sum(v, axis=0, keepdims=True)


def kernel(geo, x_refs, dy_refs, w_refs, small_refs, w_outs, r_outs, c_outs, small,
           xbuf, ybuf, part, peer, rowpart, rowpart_own, acol, brow, colpart, w_sq, msg_one, msg_two, zmsg_one, zmsg_two,
           x_sem, y_sem, first_sem, w_sem, sub_send, sub_recv, bulk_send, bulk_recv, gather_sem,
           one_send, one_recv, two_send, two_recv, z_send, z_recv, small_sem, near_sem):
    r_refs, c_refs, hyper = small[:4], small[4:8], small[8]
    n_col, n_row = geo.n_col, geo.n_row
    plane = n_col * n_row
    dp, col, row = lax.axis_index("dp"), lax.axis_index("col"), lax.axis_index("row")
    me = col * n_row + row
    own, other = dp, 1 - dp
    across = (1 - dp, col, row)
    near = ((dp, col, row + 1 - 2 * lax.rem(row, 2)), (dp, col, lax.rem(row + n_row // 2, n_row)), (dp, lax.rem(col + 1, n_col), row))

    def plane_peer(step):
        other = lax.rem(me + step, plane)
        return other, (dp, lax.div(other, n_row), lax.rem(other, n_row))

    def remote(src, dst, send, recv, device):
        return pltpu.make_async_remote_copy(
            src_ref=src, dst_ref=dst, send_sem=send, recv_sem=recv, device_id=device, device_id_type=MESH)

    def first_part(tile, j):
        r0, r_n, c0, c_n = PARTS[j]
        at = (tile, pl.ds(r0, r_n), pl.ds(c0, c_n))
        return remote(part.at[at], peer.at[at], sub_send.at[j], sub_recv.at[j], across)

    def bulk(tile):
        return remote(part.at[tile], peer.at[tile], bulk_send.at[tile], bulk_recv.at[tile], across)

    def gather(tile):
        at = (slice(None), pl.ds(pl.multiple_of(tile * TN, TN), TN))
        return remote(w_outs[0].at[at], w_outs[0].at[at], gather_sem.at[0], gather_sem.at[1], across)

    def z_copy(n, buf, slot):
        return remote(buf.at[slot], buf.at[slot], z_send.at[n], z_recv.at[n], across)

    half = geo.tokens // HALVES

    def first_x(n, pieces, c, c0, c_n):
        rows = pl.ds(c * (geo.tokens // pieces), geo.tokens // pieces)
        at = (rows, pl.ds(c0, c_n))
        return pltpu.make_async_copy(x_refs[0].at[at], xbuf.at[0].at[at], first_sem.at[n, c])

    def first_y(n, pieces, c, c0, c_n):
        rows = pl.ds(c * (geo.tokens // pieces), geo.tokens // pieces)
        columns = pl.ds(pl.multiple_of(other * TN + c0, LANES), c_n)
        return pltpu.make_async_copy(dy_refs[0].at[rows, columns], ybuf.at[0, rows, pl.ds(c0, c_n)], first_sem.at[n, c])

    n_steps = geo.n_tiles - 1

    def tile_of(s):
        past_zero = lax.div(s + (n_steps - 1), n_steps)
        past_one = lax.div(s + (n_steps - 2), n_steps)
        return s + 1 + (1 - past_zero) - (past_zero - past_one) * (2 - own)

    def slot_of(s):
        return lax.rem(s + 1, 2)

    def load(s):
        tile, slot = tile_of(s), slot_of(s)
        for first, count, m_tiles, x_ref, y_ref in geo.groups(x_refs, dy_refs):
            @pl.when(jnp.logical_and(tile >= first, tile < first + count))
            def _():
                local = tile - first
                m_at = local if m_tiles > 1 else 0
                n_at = 0 if m_tiles > 1 else local
                for h in range(HALVES):
                    rows = pl.ds(h * half, half)
                    pltpu.make_async_copy(
                        x_ref.at[rows, pl.ds(pl.multiple_of(m_at * TM, TM), TM)],
                        xbuf.at[slot, rows], x_sem.at[slot, h]).start()
                    pltpu.make_async_copy(
                        y_ref.at[rows, pl.ds(pl.multiple_of(n_at * TN, TN), TN)],
                        ybuf.at[slot, rows], y_sem.at[slot, h]).start()

    def load_done(slot, h):
        rows = pl.ds(h * half, half)
        pltpu.make_async_copy(x_refs[0].at[rows, pl.ds(0, TM)], xbuf.at[slot, rows], x_sem.at[slot, h]).wait()
        pltpu.make_async_copy(dy_refs[0].at[rows, pl.ds(0, TN)], ybuf.at[slot, rows], y_sem.at[slot, h]).wait()

    def contract(x, y):
        return lax.dot_general(x, y, (((0,), (0,)), ((), ())), preferred_element_type=F32)

    first_loads = (
        (4, lambda c: (first_x(0, 4, c, 0, 128), first_y(1, 4, c, 0, 128))),
        (2, lambda c: (first_x(2, 2, c, 128, 128),)),
        (2, lambda c: (first_y(3, 2, c, 128, 128),)),
        (2, lambda c: (first_y(4, 2, c, 256, 256),)),
    )
    for pieces, copies_of in first_loads:
        for c in range(pieces):
            for copy in copies_of(c):
                copy.start()
    load(0)

    barrier = pltpu.get_barrier_semaphore()
    for device in (across, *near):
        pl.semaphore_signal(barrier, inc=1, device_id=device, device_id_type=MESH)

    for j, (pieces, copies_of) in enumerate(first_loads):
        r0, r_n, c0, c_n = PARTS[j]
        at = (other, pl.ds(r0, r_n), pl.ds(c0, c_n))
        for c in range(pieces):
            for copy in copies_of(c):
                copy.wait()
            rows = pl.ds(c * (geo.tokens // pieces), geo.tokens // pieces)
            term = contract(xbuf[0, rows, pl.ds(r0, r_n)], ybuf[0, rows, pl.ds(c0, c_n)])
            part[at] = term if c == 0 else part[at] + term
        if j == 0:
            pl.semaphore_wait(barrier, 1 + len(near))
        first_part(other, j).start()
    w_copies = [pltpu.make_async_copy(w_refs[i], w_outs[i], w_sem.at[i]) for i in range(4)]
    w_copies += [pltpu.make_async_copy(a, b, small_sem.at[i]) for i, (a, b) in enumerate(zip(small_refs, small))]

    def tiles(lo, hi):
        @pl.loop(lo, hi)
        def _(s):
            tile, slot = tile_of(s), slot_of(s)

            @pl.when(s + 1 < n_steps)
            def _():
                load(s + 1)

            for h in range(HALVES):
                load_done(slot, h)
                rows = pl.ds(h * half, half)
                term = contract(xbuf[slot, rows, :], ybuf[slot, rows, :])
                if h == 0:
                    part[tile] = term
                else:
                    part[tile] += term

            @pl.when(s != 1)
            def _():
                bulk(tile).start()

    def w_at(i, t, r):
        if geo.wide(i):
            return pl.ds(r, RB), pl.ds(pl.multiple_of(t * TN, TN), TN)
        return pl.ds(t * TM + r, RB), pl.ds(0, TN)

    def stat_at(i, t, r):
        return pl.ds(r, RB) if geo.wide(i) else pl.ds(t * TM + r, RB)

    def stat_tile(i, t, rows_ref, accumulate, col_sum):
        tile = geo.mats[i][0] + t

        def step(b, acc):
            r = pl.multiple_of(b * RB, RB)
            grad = part[tile, pl.ds(r, RB), :] + peer[tile, pl.ds(r, RB), :]
            peer[tile, pl.ds(r, RB), :] = grad
            sq = grad * grad + EPS_ONE
            at = stat_at(i, t, r)
            if accumulate:
                rows_ref[at, :] += fold_lanes(sq)
            else:
                rows_ref[at, :] = fold_lanes(sq)
            return acc + fold_rows(sq)

        return lax.fori_loop(0, TM // RB, step, col_sum)

    def norm_tile(i, t, acc):
        tile = geo.mats[i][0] + t
        scale = brow[:, pl.ds(pl.multiple_of(t * TN, TN), TN)] if geo.wide(i) else brow[:, pl.ds(0, TN)]

        def step(b, acc):
            r = pl.multiple_of(b * RB, RB)
            upd = peer[tile, pl.ds(r, RB), :] * scale
            lane_scale = acol[stat_at(i, t, r), :]
            return acc + fold_rows(fold_lanes(upd * upd) * lane_scale * lane_scale)

        return lax.fori_loop(0, TM // RB, step, acc)

    def write_tile(i, t, step_size):
        tile = geo.mats[i][0] + t
        scale = brow[:, pl.ds(pl.multiple_of(t * TN, TN), TN)] if geo.wide(i) else brow[:, pl.ds(0, TN)]
        scale = scale * step_size

        def step(b, _):
            r = pl.multiple_of(b * RB, RB)
            upd = peer[tile, pl.ds(r, RB), :] * scale
            lane_scale = jnp.concatenate([acol[stat_at(i, t, r), :]] * (TN // LANES), axis=1)
            w_outs[i][w_at(i, t, r)] = w_outs[i][w_at(i, t, r)] - upd * lane_scale
            return 0

        lax.fori_loop(0, TM // RB, step, 0)

    def weight_squares(i):
        acc = jnp.zeros((8, LANES), F32)
        for t in range(geo.mats[i][1]):
            def step(b, acc):
                w = w_outs[i][w_at(i, t, pl.multiple_of(b * RB, RB))]
                return acc + fold_rows(fold_lanes(w * w))

            acc = lax.fori_loop(0, TM // RB, step, acc)
        w_sq[pl.ds(i, 1), :] = row_sum_of(acc)

    def row_totals(rows_ref, j):
        return row_sum_of(jnp.transpose(rows_ref[pl.ds(j, LANES), :]))

    def exchange(i, buf, send, recv):
        copies = []
        for step in range(1, plane):
            device = plane_peer(step)[1]
            copies.append(remote(buf.at[me], buf.at[me], send.at[i, step], recv.at[i, me], device))
        for copy in copies:
            copy.start()
        for step in range(1, plane):
            there, device = plane_peer(step)
            remote(buf.at[there], buf.at[there], send.at[i, step], recv.at[i, there], device).wait_recv()
        return copies

    def sizes(i):
        _, _, m_loc, n_loc = geo.mats[i]
        return m_loc, n_loc, m_loc + n_loc, m_loc * n_row, n_loc * n_col

    def round_one(i, z_part):
        m_loc, n_loc, tail, m_total, n_total = sizes(i)
        one = msg_one[i]
        r_fold = jnp.zeros((1, LANES), F32)
        for j in range(0, m_loc, LANES):
            total = row_totals(rowpart, j)
            if z_part:
                total = total + (zmsg_one[0, :, pl.ds(j, LANES)] + zmsg_one[1, :, pl.ds(j, LANES)])
            one[pl.ds(me, 1), :, pl.ds(j, LANES)] = total[None]
            r_fold = r_fold + r_refs[i][:, pl.ds(j, LANES)]
        one[pl.ds(me, 1), :, pl.ds(m_loc, n_loc)] = colpart[:, pl.ds(0, n_loc)][None]
        if z_part:
            for t in range(2):
                one[pl.ds(me, 1), :, pl.ds(m_loc + t * TN, TN)] = zmsg_one[t, :, pl.ds(m_loc, TN)][None]
        one[pl.ds(me, 1), :, pl.ds(tail, LANES)] = r_fold[None]
        one[pl.ds(me, 1), :, pl.ds(tail + LANES, LANES)] = w_sq[pl.ds(i, 1), :][None]
        sent = exchange(i, one, one_send, one_recv)

        row_sum = one[row, :, pl.ds(0, m_loc)]
        for j in range(1, n_col):
            row_sum = row_sum + one[j * n_row + row, :, pl.ds(0, m_loc)]
        col_sum = one[col * n_row, :, pl.ds(m_loc, n_loc)]
        for j in range(1, n_row):
            col_sum = col_sum + one[col * n_row + j, :, pl.ds(m_loc, n_loc)]
        new_row = beta_two * r_refs[i][...] + (1.0 - beta_two) * (row_sum / n_total)
        new_col = beta_two * c_refs[i][...] + (1.0 - beta_two) * (col_sum / m_total)
        r_outs[i][...] = new_row
        c_outs[i][...] = new_col

        old_fold = jnp.zeros((1, LANES), F32)
        sq_fold = jnp.zeros((1, LANES), F32)
        for j in range(plane):
            sq_fold = sq_fold + fold_lanes(one[j, :, pl.ds(0, m_loc)])
            if j < n_row:
                old_fold = old_fold + one[j, :, pl.ds(tail, LANES)]
        total = lane_sum(beta_two * old_fold + (1.0 - beta_two) * (sq_fold / n_total))

        row_scale = 1.0 / jnp.sqrt(new_row / total)
        for j in range(0, m_loc, LANES):
            acol[pl.ds(j, LANES), :] = jnp.transpose(jnp.broadcast_to(row_scale[:, j:j + LANES], (LANES, LANES)))
        brow[:, pl.ds(0, n_loc)] = 1.0 / jnp.sqrt(new_col)
        return sent

    def round_two(i, upd_sq):
        _, _, tail, m_total, n_total = sizes(i)
        one, two = msg_one[i], msg_two.at[i]
        two[pl.ds(me, 1)] = upd_sq[None]
        sent = exchange(i, two, two_send, two_recv)
        upd_fold, w_fold = two[0], one[0, :, pl.ds(tail + LANES, LANES)]
        for j in range(1, plane):
            upd_fold = upd_fold + two[j]
            w_fold = w_fold + one[j, :, pl.ds(tail + LANES, LANES)]
        upd_rms = jnp.sqrt(lane_sum(upd_fold) / (m_total * n_total))
        w_rms = jnp.sqrt(lane_sum(w_fold) / (m_total * n_total))
        return rho_step * jnp.maximum(EPS_TWO, w_rms) / jnp.maximum(1.0, upd_rms / clip_thr), sent

    none = jnp.zeros((8, TN), F32)
    no_lanes = jnp.zeros((8, LANES), F32)
    m_gate = geo.mats[0][2]

    tiles(0, 4)

    for copy in w_copies:
        copy.start()

    for n in range(2):
        for device in near:
            pl.semaphore_signal(near_sem.at[n], inc=1, device_id=device, device_id_type=MESH)
        pl.semaphore_wait(near_sem.at[n], len(near))

    for copy in w_copies:
        copy.wait()
    beta_two, rho_step, clip_thr = hyper[0], hyper[1], hyper[2]
    for i in range(4):
        weight_squares(i)
    for j in range(len(PARTS)):
        first_part(own, j).wait_recv()
    own_col = stat_tile(0, own, rowpart_own, False, none)
    for j in range(0, TM, LANES):
        zmsg_one[pl.ds(own, 1), :, pl.ds(j, LANES)] = row_totals(rowpart_own, j)[None]
    zmsg_one[pl.ds(own, 1), :, pl.ds(m_gate, TN)] = row_sum_of(own_col)[None]
    z_copy(0, zmsg_one, own).start()

    tiles(4, 6)

    shared = range(2, geo.mats[0][1])
    for t in shared:
        bulk(t).wait_recv()
        colpart[:, pl.ds(t * TN, TN)] = row_sum_of(stat_tile(0, t, rowpart, t > 2, none))
    z_copy(0, zmsg_one, other).wait_recv()
    gate_sent = round_one(0, True)
    zmsg_two[pl.ds(own, 1)] = row_sum_of(norm_tile(0, own, no_lanes))[None]
    z_copy(1, zmsg_two, own).start()

    tiles(6, 8)

    upd_sq = no_lanes
    for t in shared:
        upd_sq = norm_tile(0, t, upd_sq)
    z_copy(1, zmsg_two, other).wait_recv()
    step_size, sent = round_two(0, row_sum_of(upd_sq) + (zmsg_two[0] + zmsg_two[1]))
    gate_sent += sent
    write_tile(0, own, step_size)
    for t in shared:
        write_tile(0, t, step_size)

    tiles(8, geo.n_tiles - 1)
    gather(own).start()

    for i in range(1, 4):
        first, count, m_loc, n_loc = geo.mats[i]
        col_sum = none
        for t in range(count):
            bulk(first + t).wait_recv()
            if geo.wide(i):
                colpart[:, pl.ds(t * TN, TN)] = row_sum_of(stat_tile(i, t, rowpart, t > 0, none))
            else:
                col_sum = stat_tile(i, t, rowpart, False, col_sum)
        if not geo.wide(i):
            colpart[:, pl.ds(0, TN)] = row_sum_of(col_sum)
        sent_one = round_one(i, False)
        upd_sq = no_lanes
        for t in range(count):
            upd_sq = norm_tile(i, t, upd_sq)
        step_size, sent_two = round_two(i, row_sum_of(upd_sq))
        for t in range(count):
            write_tile(i, t, step_size)
        for copy in sent_one + sent_two:
            copy.wait_send()

    for copy in gate_sent:
        copy.wait_send()
    z_copy(0, zmsg_one, own).wait_send()
    z_copy(1, zmsg_two, own).wait_send()
    for j in range(len(PARTS)):
        first_part(other, j).wait_send()

    @pl.loop(2, geo.n_tiles)
    def _(tile):
        bulk(tile).wait_send()

    gather(own).wait_send()
    gather(other).wait_recv()


def write_out(*refs):
    copies = [pltpu.make_async_copy(refs[i], refs[12 + i], refs[24].at[i]) for i in range(12)]
    for copy in copies:
        copy.start()
    for copy in copies:
        copy.wait()


class Geometry:
    def __init__(self, n_row, n_col, tokens, blocks):
        self.n_row, self.n_col = n_row, n_col
        self.tokens = tokens
        self.mats, first = [], 0
        for m_loc, n_loc in blocks:
            count = (m_loc // TM) * (n_loc // TN)
            self.mats.append((first, count, m_loc, n_loc))
            first += count
        self.n_tiles = first

    def wide(self, i):
        return self.mats[i][2] == TM

    def groups(self, x_refs, dy_refs):
        for (first, count, m_loc, _), x_ref, y_ref in zip(self.mats, x_refs, dy_refs):
            yield first, count, m_loc // TM, x_ref, y_ref


def solution(mesh):
    n_row, n_col = mesh.shape["row"], mesh.shape["col"]
    plane = n_row * n_col
    act_spec = P('dp', 'row')
    grad_spec = P('dp', 'col')
    w_spec = P('row', 'col')
    row_spec = P('row')
    col_spec = P('col')
    in_specs = (act_spec, grad_spec, act_spec, grad_spec, grad_spec, act_spec, grad_spec,
                w_spec, w_spec, w_spec, w_spec,
                row_spec, col_spec, row_spec, col_spec, row_spec, col_spec, row_spec, col_spec, P())
    out_specs = (w_spec, row_spec, col_spec) * 4

    def per_device(x_attn, dy_attn, x_mlp, dy_gate, dy_up, h_mlp, dy_out, w_attn, w_gate, w_up, w_down,
                   r_attn, c_attn, r_gate, c_gate, r_up, c_up, r_down, c_down, hyper_params):
        weights = (w_gate, w_up, w_down, w_attn)
        rows = [v.reshape(1, -1) for v in (r_gate, r_up, r_down, r_attn)]
        cols = [v.reshape(1, -1) for v in (c_gate, c_up, c_down, c_attn)]
        blocks = [w.shape for w in weights]
        geo = Geometry(n_row, n_col, x_attn.shape[0], blocks)
        results = (*weights, *rows, *cols)
        hbm = pl.BlockSpec(memory_space=pl.ANY)
        vmem = pl.BlockSpec(memory_space=pltpu.VMEM)
        dma = pltpu.SemaphoreType.DMA
        max_m, max_n = max(b[0] for b in blocks), max(b[1] for b in blocks)

        def body(*refs):
            xs = (refs[0], refs[0], refs[1], refs[2])
            kernel(geo, xs, refs[3:7], refs[7:11], refs[11:20], refs[20:24], refs[24:28], refs[28:32], refs[32:41],
                   *refs[41:51], refs[51:55], *refs[55:])

        outs = pl.pallas_call(
            body,
            out_shape=tuple(pltpu.VMEM(v.shape, F32) for v in results),
            in_specs=[hbm] * 20,
            out_specs=(vmem,) * 12,
            scratch_shapes=[pltpu.VMEM(v.shape, F32) for v in (*rows, *cols)] + [
                pltpu.SMEM((3,), F32),
                pltpu.VMEM((2, geo.tokens, TM), jnp.bfloat16),
                pltpu.VMEM((2, geo.tokens, TN), jnp.bfloat16),
                pltpu.VMEM((geo.n_tiles, TM, TN), F32),
                pltpu.VMEM((geo.n_tiles, TM, TN), F32),
                pltpu.VMEM((max_m, LANES), F32),
                pltpu.VMEM((TM, LANES), F32),
                pltpu.VMEM((max_m, LANES), F32),
                pltpu.VMEM((1, max_n), F32),
                pltpu.VMEM((1, max_n), F32),
                pltpu.VMEM((8, LANES), F32),
            ] + [pltpu.VMEM((plane, 1, m + n + 2 * LANES), F32) for m, n in blocks] + [
                pltpu.VMEM((4, plane, 1, LANES), F32),
                pltpu.VMEM((2, 1, TM + TN), F32),
                pltpu.VMEM((2, 1, LANES), F32),
                dma((2, HALVES)), dma((2, HALVES)), dma((5, 4)), dma((4,)),
                dma((len(PARTS),)), dma((len(PARTS),)), dma((geo.n_tiles,)), dma((geo.n_tiles,)), dma((2,)),
                dma((4, plane)), dma((4, plane)), dma((4, plane)), dma((4, plane)), dma((2,)), dma((2,)), dma((9,)),
                pltpu.SemaphoreType.REGULAR((2,)),
            ],
            compiler_params=pltpu.CompilerParams(
                collective_id=0, has_side_effects=True, vmem_limit_bytes=48 << 20),
            name="adafactor_step",
        )(x_mlp, h_mlp, x_attn, dy_gate, dy_up, dy_out, dy_attn, *weights, *rows, *cols, hyper_params)
        outs = pl.pallas_call(
            write_out,
            out_shape=tuple(jax.ShapeDtypeStruct(v.shape, F32) for v in results),
            in_specs=[vmem] * 12,
            out_specs=(hbm,) * 12,
            scratch_shapes=[dma((12,))],
            compiler_params=pltpu.CompilerParams(vmem_limit_bytes=1 << 20),
            name="write_out",
        )(*[pltpu.with_memory_space_constraint(v, pltpu.VMEM) for v in outs])
        w_new, r_new, c_new = outs[:4], outs[4:8], outs[8:]
        result = []
        for i in (3, 0, 1, 2):
            result += [w_new[i], r_new[i].reshape(-1), c_new[i].reshape(-1)]
        return tuple(result)

    return jax.shard_map(per_device, mesh=mesh, in_specs=in_specs, out_specs=out_specs, check_vma=False)
```

```python
import jax
import jax.numpy as jnp
from jax import lax
from jax.experimental import pallas as pl
from jax.experimental.pallas import tpu as pltpu
from jax.sharding import PartitionSpec as P

EPS_ONE = 1e-30
EPS_TWO = 1e-3
MESH = pl.DeviceIdType.MESH
F32 = jnp.float32

TM, TN = 256, 512
HALVES = 2
PARTS = ((0, 128, 0, 128), (0, 128, 128, 128), (128, 128, 0, 256), (0, 256, 256, 256))
RB = 32
LANES = 128


def fold_lanes(v):
    total = v[:, :LANES]
    for j in range(LANES, v.shape[1], LANES):
        total = total + v[:, j:j + LANES]
    return total


def fold_rows(v):
    total = v[:8]
    for i in range(8, v.shape[0], 8):
        total = total + v[i:i + 8]
    return total


def lane_sum(v):
    return jnp.sum(v, axis=1, keepdims=True)


def row_sum_of(v):
    return jnp.sum(v, axis=0, keepdims=True)


def kernel(geo, x_refs, dy_refs, w_refs, small_refs, w_outs, r_outs, c_outs, small,
           xbuf, ybuf, part, peer, rowpart, rowpart_own, acol, brow, colpart, w_sq, msg_one, msg_two, zmsg_one, zmsg_two,
           x_sem, y_sem, first_sem, w_sem, sub_send, sub_recv, bulk_send, bulk_recv, gather_sem,
           one_send, one_recv, two_send, two_recv, z_send, z_recv, small_sem, near_sem):
    r_refs, c_refs, hyper = small[:4], small[4:8], small[8]
    n_col, n_row = geo.n_col, geo.n_row
    plane = n_col * n_row
    dp, col, row = lax.axis_index("dp"), lax.axis_index("col"), lax.axis_index("row")
    me = col * n_row + row
    own, other = dp, 1 - dp
    across = (1 - dp, col, row)
    near = ((dp, col, row + 1 - 2 * lax.rem(row, 2)), (dp, col, lax.rem(row + n_row // 2, n_row)), (dp, lax.rem(col + 1, n_col), row))

    def plane_peer(step):
        other = lax.rem(me + step, plane)
        return other, (dp, lax.div(other, n_row), lax.rem(other, n_row))

    def remote(src, dst, send, recv, device):
        return pltpu.make_async_remote_copy(
            src_ref=src, dst_ref=dst, send_sem=send, recv_sem=recv, device_id=device, device_id_type=MESH)

    def first_part(tile, j):
        r0, r_n, c0, c_n = PARTS[j]
        at = (tile, pl.ds(r0, r_n), pl.ds(c0, c_n))
        return remote(part.at[at], peer.at[at], sub_send.at[j], sub_recv.at[j], across)

    def bulk(tile):
        return remote(part.at[tile], peer.at[tile], bulk_send.at[tile], bulk_recv.at[tile], across)

    def gather(tile):
        at = (slice(None), pl.ds(pl.multiple_of(tile * TN, TN), TN))
        return remote(w_outs[0].at[at], w_outs[0].at[at], gather_sem.at[0], gather_sem.at[1], across)

    def z_copy(n, buf, slot):
        return remote(buf.at[slot], buf.at[slot], z_send.at[n], z_recv.at[n], across)

    barrier = pltpu.get_barrier_semaphore()
    for device in (across, *near):
        pl.semaphore_signal(barrier, inc=1, device_id=device, device_id_type=MESH)

    half = geo.tokens // HALVES

    def first_x(n, pieces, c, c0, c_n):
        rows = pl.ds(c * (geo.tokens // pieces), geo.tokens // pieces)
        at = (rows, pl.ds(c0, c_n))
        return pltpu.make_async_copy(x_refs[0].at[at], xbuf.at[0].at[at], first_sem.at[n, c])

    def first_y(n, pieces, c, c0, c_n):
        rows = pl.ds(c * (geo.tokens // pieces), geo.tokens // pieces)
        columns = pl.ds(pl.multiple_of(other * TN + c0, LANES), c_n)
        return pltpu.make_async_copy(dy_refs[0].at[rows, columns], ybuf.at[0, rows, pl.ds(c0, c_n)], first_sem.at[n, c])

    n_steps = geo.n_tiles - 1

    def tile_of(s):
        past_zero = lax.div(s + (n_steps - 1), n_steps)
        past_one = lax.div(s + (n_steps - 2), n_steps)
        return s + 1 + (1 - past_zero) - (past_zero - past_one) * (2 - own)

    def slot_of(s):
        return lax.rem(s + 1, 2)

    def load(s):
        tile, slot = tile_of(s), slot_of(s)
        for first, count, m_tiles, x_ref, y_ref in geo.groups(x_refs, dy_refs):
            @pl.when(jnp.logical_and(tile >= first, tile < first + count))
            def _():
                local = tile - first
                m_at = local if m_tiles > 1 else 0
                n_at = 0 if m_tiles > 1 else local
                for h in range(HALVES):
                    rows = pl.ds(h * half, half)
                    pltpu.make_async_copy(
                        x_ref.at[rows, pl.ds(pl.multiple_of(m_at * TM, TM), TM)],
                        xbuf.at[slot, rows], x_sem.at[slot, h]).start()
                    pltpu.make_async_copy(
                        y_ref.at[rows, pl.ds(pl.multiple_of(n_at * TN, TN), TN)],
                        ybuf.at[slot, rows], y_sem.at[slot, h]).start()

    def load_done(slot, h):
        rows = pl.ds(h * half, half)
        pltpu.make_async_copy(x_refs[0].at[rows, pl.ds(0, TM)], xbuf.at[slot, rows], x_sem.at[slot, h]).wait()
        pltpu.make_async_copy(dy_refs[0].at[rows, pl.ds(0, TN)], ybuf.at[slot, rows], y_sem.at[slot, h]).wait()

    def contract(x, y):
        return lax.dot_general(x, y, (((0,), (0,)), ((), ())), preferred_element_type=F32)

    first_loads = (
        (4, lambda c: (first_x(0, 4, c, 0, 128), first_y(1, 4, c, 0, 128))),
        (2, lambda c: (first_y(2, 2, c, 128, 128),)),
        (2, lambda c: (first_x(3, 2, c, 128, 128),)),
        (2, lambda c: (first_y(4, 2, c, 256, 256),)),
    )
    def start_first(j):
        pieces, copies_of = first_loads[j]
        for c in range(pieces):
            for copy in copies_of(c):
                copy.start()

    for j in range(4):
        start_first(j)
    starts = {(2, 0): lambda: load(0)}

    for j, (pieces, copies_of) in enumerate(first_loads):
        r0, r_n, c0, c_n = PARTS[j]
        at = (other, pl.ds(r0, r_n), pl.ds(c0, c_n))
        for c in range(pieces):
            for copy in copies_of(c):
                copy.wait()
            if (j, c) in starts:
                starts[j, c]()
            rows = pl.ds(c * (geo.tokens // pieces), geo.tokens // pieces)
            term = contract(xbuf[0, rows, pl.ds(r0, r_n)], ybuf[0, rows, pl.ds(c0, c_n)])
            part[at] = term if c == 0 else part[at] + term
        if j == 0:
            pl.semaphore_wait(barrier, 1 + len(near))
        if j in (2,):
            @pl.when(lax.rem(row, 2) == 0)
            def _():
                first_part(other, j).start()
        else:
            if j == 3:
                @pl.when(lax.rem(row, 2) == 1)
                def _():
                    for held in (2,):
                        first_part(other, held).start()
            first_part(other, j).start()
    w_copies = [pltpu.make_async_copy(w_refs[i], w_outs[i], w_sem.at[i]) for i in range(4)]
    w_copies += [pltpu.make_async_copy(a, b, small_sem.at[i]) for i, (a, b) in enumerate(zip(small_refs, small))]

    def tiles(lo, hi):
        @pl.loop(lo, hi)
        def _(s):
            tile, slot = tile_of(s), slot_of(s)

            @pl.when(s + 1 < n_steps)
            def _():
                load(s + 1)

            for h in range(HALVES):
                load_done(slot, h)
                rows = pl.ds(h * half, half)
                term = contract(xbuf[slot, rows, :], ybuf[slot, rows, :])
                if h == 0:
                    part[tile] = term
                else:
                    part[tile] += term

            @pl.when(s != 1)
            def _():
                bulk(tile).start()

    def w_at(i, t, r):
        if geo.wide(i):
            return pl.ds(r, RB), pl.ds(pl.multiple_of(t * TN, TN), TN)
        return pl.ds(t * TM + r, RB), pl.ds(0, TN)

    def stat_at(i, t, r):
        return pl.ds(r, RB) if geo.wide(i) else pl.ds(t * TM + r, RB)

    def stat_tile(i, t, rows_ref, accumulate, col_sum):
        tile = geo.mats[i][0] + t

        def step(b, acc):
            r = pl.multiple_of(b * RB, RB)
            grad = part[tile, pl.ds(r, RB), :] + peer[tile, pl.ds(r, RB), :]
            peer[tile, pl.ds(r, RB), :] = grad
            sq = grad * grad + EPS_ONE
            at = stat_at(i, t, r)
            if accumulate:
                rows_ref[at, :] += fold_lanes(sq)
            else:
                rows_ref[at, :] = fold_lanes(sq)
            return acc + fold_rows(sq)

        return lax.fori_loop(0, TM // RB, step, col_sum)

    def norm_tile(i, t, acc):
        tile = geo.mats[i][0] + t
        scale = brow[:, pl.ds(pl.multiple_of(t * TN, TN), TN)] if geo.wide(i) else brow[:, pl.ds(0, TN)]

        def step(b, acc):
            r = pl.multiple_of(b * RB, RB)
            upd = peer[tile, pl.ds(r, RB), :] * scale
            lane_scale = acol[stat_at(i, t, r), :]
            return acc + fold_rows(fold_lanes(upd * upd) * lane_scale * lane_scale)

        return lax.fori_loop(0, TM // RB, step, acc)

    def write_tile(i, t, step_size):
        tile = geo.mats[i][0] + t
        scale = brow[:, pl.ds(pl.multiple_of(t * TN, TN), TN)] if geo.wide(i) else brow[:, pl.ds(0, TN)]
        scale = scale * step_size

        def step(b, _):
            r = pl.multiple_of(b * RB, RB)
            upd = peer[tile, pl.ds(r, RB), :] * scale
            lane_scale = jnp.concatenate([acol[stat_at(i, t, r), :]] * (TN // LANES), axis=1)
            w_outs[i][w_at(i, t, r)] = w_outs[i][w_at(i, t, r)] - upd * lane_scale
            return 0

        lax.fori_loop(0, TM // RB, step, 0)

    def weight_squares(i):
        acc = jnp.zeros((8, LANES), F32)
        for t in range(geo.mats[i][1]):
            def step(b, acc):
                w = w_outs[i][w_at(i, t, pl.multiple_of(b * RB, RB))]
                return acc + fold_rows(fold_lanes(w * w))

            acc = lax.fori_loop(0, TM // RB, step, acc)
        w_sq[pl.ds(i, 1), :] = row_sum_of(acc)

    def row_totals(rows_ref, j):
        return row_sum_of(jnp.transpose(rows_ref[pl.ds(j, LANES), :]))

    def exchange(i, buf, send, recv):
        copies = []
        for step in range(1, plane):
            device = plane_peer(step)[1]
            copies.append(remote(buf.at[me], buf.at[me], send.at[i, step], recv.at[i, me], device))
        for copy in copies:
            copy.start()
        for step in range(1, plane):
            there, device = plane_peer(step)
            remote(buf.at[there], buf.at[there], send.at[i, step], recv.at[i, there], device).wait_recv()
        return copies

    def sizes(i):
        _, _, m_loc, n_loc = geo.mats[i]
        return m_loc, n_loc, m_loc + n_loc, m_loc * n_row, n_loc * n_col

    def round_one(i, z_part):
        m_loc, n_loc, tail, m_total, n_total = sizes(i)
        one = msg_one[i]
        r_fold = jnp.zeros((1, LANES), F32)
        for j in range(0, m_loc, LANES):
            total = row_totals(rowpart, j)
            if z_part:
                total = total + (zmsg_one[0, :, pl.ds(j, LANES)] + zmsg_one[1, :, pl.ds(j, LANES)])
            one[pl.ds(me, 1), :, pl.ds(j, LANES)] = total[None]
            r_fold = r_fold + r_refs[i][:, pl.ds(j, LANES)]
        one[pl.ds(me, 1), :, pl.ds(m_loc, n_loc)] = colpart[:, pl.ds(0, n_loc)][None]
        if z_part:
            for t in range(2):
                one[pl.ds(me, 1), :, pl.ds(m_loc + t * TN, TN)] = zmsg_one[t, :, pl.ds(m_loc, TN)][None]
        one[pl.ds(me, 1), :, pl.ds(tail, LANES)] = r_fold[None]
        one[pl.ds(me, 1), :, pl.ds(tail + LANES, LANES)] = w_sq[pl.ds(i, 1), :][None]
        sent = exchange(i, one, one_send, one_recv)

        row_sum = one[row, :, pl.ds(0, m_loc)]
        for j in range(1, n_col):
            row_sum = row_sum + one[j * n_row + row, :, pl.ds(0, m_loc)]
        col_sum = one[col * n_row, :, pl.ds(m_loc, n_loc)]
        for j in range(1, n_row):
            col_sum = col_sum + one[col * n_row + j, :, pl.ds(m_loc, n_loc)]
        new_row = beta_two * r_refs[i][...] + (1.0 - beta_two) * (row_sum / n_total)
        new_col = beta_two * c_refs[i][...] + (1.0 - beta_two) * (col_sum / m_total)
        r_outs[i][...] = new_row
        c_outs[i][...] = new_col

        old_fold = jnp.zeros((1, LANES), F32)
        sq_fold = jnp.zeros((1, LANES), F32)
        for j in range(plane):
            sq_fold = sq_fold + fold_lanes(one[j, :, pl.ds(0, m_loc)])
            if j < n_row:
                old_fold = old_fold + one[j, :, pl.ds(tail, LANES)]
        total = lane_sum(beta_two * old_fold + (1.0 - beta_two) * (sq_fold / n_total))

        row_scale = 1.0 / jnp.sqrt(new_row / total)
        for j in range(0, m_loc, LANES):
            acol[pl.ds(j, LANES), :] = jnp.transpose(jnp.broadcast_to(row_scale[:, j:j + LANES], (LANES, LANES)))
        brow[:, pl.ds(0, n_loc)] = 1.0 / jnp.sqrt(new_col)
        return sent

    def round_two(i, upd_sq):
        _, _, tail, m_total, n_total = sizes(i)
        one, two = msg_one[i], msg_two.at[i]
        two[pl.ds(me, 1)] = upd_sq[None]
        sent = exchange(i, two, two_send, two_recv)
        upd_fold, w_fold = two[0], one[0, :, pl.ds(tail + LANES, LANES)]
        for j in range(1, plane):
            upd_fold = upd_fold + two[j]
            w_fold = w_fold + one[j, :, pl.ds(tail + LANES, LANES)]
        upd_rms = jnp.sqrt(lane_sum(upd_fold) / (m_total * n_total))
        w_rms = jnp.sqrt(lane_sum(w_fold) / (m_total * n_total))
        return rho_step * jnp.maximum(EPS_TWO, w_rms) / jnp.maximum(1.0, upd_rms / clip_thr), sent

    none = jnp.zeros((8, TN), F32)
    no_lanes = jnp.zeros((8, LANES), F32)
    m_gate = geo.mats[0][2]

    tiles(0, 4)

    for copy in w_copies:
        copy.start()

    for n in range(2):
        for device in near:
            pl.semaphore_signal(near_sem.at[n], inc=1, device_id=device, device_id_type=MESH)
        pl.semaphore_wait(near_sem.at[n], len(near))

    for copy in w_copies:
        copy.wait()
    beta_two, rho_step, clip_thr = hyper[0], hyper[1], hyper[2]
    for i in range(4):
        weight_squares(i)
    for j in range(len(PARTS)):
        first_part(own, j).wait_recv()
    own_col = stat_tile(0, own, rowpart_own, False, none)
    for j in range(0, TM, LANES):
        zmsg_one[pl.ds(own, 1), :, pl.ds(j, LANES)] = row_totals(rowpart_own, j)[None]
    zmsg_one[pl.ds(own, 1), :, pl.ds(m_gate, TN)] = row_sum_of(own_col)[None]
    z_copy(0, zmsg_one, own).start()

    tiles(4, 6)

    shared = range(2, geo.mats[0][1])
    for t in shared:
        bulk(t).wait_recv()
        colpart[:, pl.ds(t * TN, TN)] = row_sum_of(stat_tile(0, t, rowpart, t > 2, none))
    z_copy(0, zmsg_one, other).wait_recv()
    gate_sent = round_one(0, True)
    zmsg_two[pl.ds(own, 1)] = row_sum_of(norm_tile(0, own, no_lanes))[None]
    z_copy(1, zmsg_two, own).start()

    tiles(6, 8)

    upd_sq = no_lanes
    for t in shared:
        upd_sq = norm_tile(0, t, upd_sq)
    z_copy(1, zmsg_two, other).wait_recv()
    step_size, sent = round_two(0, row_sum_of(upd_sq) + (zmsg_two[0] + zmsg_two[1]))
    gate_sent += sent
    write_tile(0, own, step_size)
    for t in shared:
        write_tile(0, t, step_size)

    tiles(8, geo.n_tiles - 1)
    gather(own).start()

    for i in range(1, 4):
        first, count, m_loc, n_loc = geo.mats[i]
        col_sum = none
        for t in range(count):
            bulk(first + t).wait_recv()
            if geo.wide(i):
                colpart[:, pl.ds(t * TN, TN)] = row_sum_of(stat_tile(i, t, rowpart, t > 0, none))
            else:
                col_sum = stat_tile(i, t, rowpart, False, col_sum)
        if not geo.wide(i):
            colpart[:, pl.ds(0, TN)] = row_sum_of(col_sum)
        sent_one = round_one(i, False)
        upd_sq = no_lanes
        for t in range(count):
            upd_sq = norm_tile(i, t, upd_sq)
        step_size, sent_two = round_two(i, row_sum_of(upd_sq))
        for t in range(count):
            write_tile(i, t, step_size)
        for copy in sent_one + sent_two:
            copy.wait_send()

    for copy in gate_sent:
        copy.wait_send()
    z_copy(0, zmsg_one, own).wait_send()
    z_copy(1, zmsg_two, own).wait_send()
    for j in range(len(PARTS)):
        first_part(other, j).wait_send()

    @pl.loop(2, geo.n_tiles)
    def _(tile):
        bulk(tile).wait_send()

    gather(own).wait_send()
    gather(other).wait_recv()


def write_out(*refs):
    copies = [pltpu.make_async_copy(refs[i], refs[12 + i], refs[24].at[i]) for i in range(12)]
    for copy in copies:
        copy.start()
    for copy in copies:
        copy.wait()


class Geometry:
    def __init__(self, n_row, n_col, tokens, blocks):
        self.n_row, self.n_col = n_row, n_col
        self.tokens = tokens
        self.mats, first = [], 0
        for m_loc, n_loc in blocks:
            count = (m_loc // TM) * (n_loc // TN)
            self.mats.append((first, count, m_loc, n_loc))
            first += count
        self.n_tiles = first

    def wide(self, i):
        return self.mats[i][2] == TM

    def groups(self, x_refs, dy_refs):
        for (first, count, m_loc, _), x_ref, y_ref in zip(self.mats, x_refs, dy_refs):
            yield first, count, m_loc // TM, x_ref, y_ref


def solution(mesh):
    n_row, n_col = mesh.shape["row"], mesh.shape["col"]
    plane = n_row * n_col
    act_spec = P('dp', 'row')
    grad_spec = P('dp', 'col')
    w_spec = P('row', 'col')
    row_spec = P('row')
    col_spec = P('col')
    in_specs = (act_spec, grad_spec, act_spec, grad_spec, grad_spec, act_spec, grad_spec,
                w_spec, w_spec, w_spec, w_spec,
                row_spec, col_spec, row_spec, col_spec, row_spec, col_spec, row_spec, col_spec, P())
    out_specs = (w_spec, row_spec, col_spec) * 4

    def per_device(x_attn, dy_attn, x_mlp, dy_gate, dy_up, h_mlp, dy_out, w_attn, w_gate, w_up, w_down,
                   r_attn, c_attn, r_gate, c_gate, r_up, c_up, r_down, c_down, hyper_params):
        weights = (w_gate, w_up, w_down, w_attn)
        rows = [v.reshape(1, -1) for v in (r_gate, r_up, r_down, r_attn)]
        cols = [v.reshape(1, -1) for v in (c_gate, c_up, c_down, c_attn)]
        blocks = [w.shape for w in weights]
        geo = Geometry(n_row, n_col, x_attn.shape[0], blocks)
        results = (*weights, *rows, *cols)
        hbm = pl.BlockSpec(memory_space=pl.ANY)
        vmem = pl.BlockSpec(memory_space=pltpu.VMEM)
        dma = pltpu.SemaphoreType.DMA
        max_m, max_n = max(b[0] for b in blocks), max(b[1] for b in blocks)

        def body(*refs):
            xs = (refs[0], refs[0], refs[1], refs[2])
            kernel(geo, xs, refs[3:7], refs[7:11], refs[11:20], refs[20:24], refs[24:28], refs[28:32], refs[32:41],
                   *refs[41:51], refs[51:55], *refs[55:])

        outs = pl.pallas_call(
            body,
            out_shape=tuple(pltpu.VMEM(v.shape, F32) for v in results),
            in_specs=[hbm] * 20,
            out_specs=(vmem,) * 12,
            scratch_shapes=[pltpu.VMEM(v.shape, F32) for v in (*rows, *cols)] + [
                pltpu.SMEM((3,), F32),
                pltpu.VMEM((2, geo.tokens, TM), jnp.bfloat16),
                pltpu.VMEM((2, geo.tokens, TN), jnp.bfloat16),
                pltpu.VMEM((geo.n_tiles, TM, TN), F32),
                pltpu.VMEM((geo.n_tiles, TM, TN), F32),
                pltpu.VMEM((max_m, LANES), F32),
                pltpu.VMEM((TM, LANES), F32),
                pltpu.VMEM((max_m, LANES), F32),
                pltpu.VMEM((1, max_n), F32),
                pltpu.VMEM((1, max_n), F32),
                pltpu.VMEM((8, LANES), F32),
            ] + [pltpu.VMEM((plane, 1, m + n + 2 * LANES), F32) for m, n in blocks] + [
                pltpu.VMEM((4, plane, 1, LANES), F32),
                pltpu.VMEM((2, 1, TM + TN), F32),
                pltpu.VMEM((2, 1, LANES), F32),
                dma((2, HALVES)), dma((2, HALVES)), dma((5, 4)), dma((4,)),
                dma((len(PARTS),)), dma((len(PARTS),)), dma((geo.n_tiles,)), dma((geo.n_tiles,)), dma((2,)),
                dma((4, plane)), dma((4, plane)), dma((4, plane)), dma((4, plane)), dma((2,)), dma((2,)), dma((9,)),
                pltpu.SemaphoreType.REGULAR((2,)),
            ],
            compiler_params=pltpu.CompilerParams(
                collective_id=0, has_side_effects=True, vmem_limit_bytes=48 << 20),
            name="adafactor_step",
        )(x_mlp, h_mlp, x_attn, dy_gate, dy_up, dy_out, dy_attn, *weights, *rows, *cols, hyper_params)
        outs = pl.pallas_call(
            write_out,
            out_shape=tuple(jax.ShapeDtypeStruct(v.shape, F32) for v in results),
            in_specs=[vmem] * 12,
            out_specs=(hbm,) * 12,
            scratch_shapes=[dma((12,))],
            compiler_params=pltpu.CompilerParams(vmem_limit_bytes=1 << 20),
            name="write_out",
        )(*[pltpu.with_memory_space_constraint(v, pltpu.VMEM) for v in outs])
        w_new, r_new, c_new = outs[:4], outs[4:8], outs[8:]
        result = []
        for i in (3, 0, 1, 2):
            result += [w_new[i], r_new[i].reshape(-1), c_new[i].reshape(-1)]
        return tuple(result)

    return jax.shard_map(per_device, mesh=mesh, in_specs=in_specs, out_specs=out_specs, check_vma=False)
```

```python
import jax
import jax.numpy as jnp
from jax import lax
from jax.experimental import pallas as pl
from jax.experimental.pallas import tpu as pltpu
from jax.sharding import PartitionSpec as P

EPS_ONE = 1e-30
EPS_TWO = 1e-3
MESH = pl.DeviceIdType.MESH
F32 = jnp.float32

TM, TN = 256, 512
HALVES = 2
PARTS = ((0, 128, 0, 128), (0, 128, 128, 128), (128, 128, 0, 256), (0, 256, 256, 256))
RB = 32
LANES = 128


def fold_lanes(v):
    total = v[:, :LANES]
    for j in range(LANES, v.shape[1], LANES):
        total = total + v[:, j:j + LANES]
    return total


def fold_rows(v):
    total = v[:8]
    for i in range(8, v.shape[0], 8):
        total = total + v[i:i + 8]
    return total


def lane_sum(v):
    return jnp.sum(v, axis=1, keepdims=True)


def row_sum_of(v):
    return jnp.sum(v, axis=0, keepdims=True)


def kernel(geo, x_refs, dy_refs, w_refs, small_refs, w_outs, r_outs, c_outs, small,
           xbuf, ybuf, part, peer, rowpart, rowpart_own, acol, brow, colpart, w_sq, msg_one, msg_two, zmsg_one, zmsg_two,
           x_sem, y_sem, first_sem, w_sem, sub_send, sub_recv, bulk_send, bulk_recv, gather_sem,
           one_send, one_recv, two_send, two_recv, z_send, z_recv, small_sem, near_sem):
    r_refs, c_refs, hyper = small[:4], small[4:8], small[8]
    n_col, n_row = geo.n_col, geo.n_row
    plane = n_col * n_row
    dp, col, row = lax.axis_index("dp"), lax.axis_index("col"), lax.axis_index("row")
    me = col * n_row + row
    own, other = dp, 1 - dp
    across = (1 - dp, col, row)
    near = ((dp, col, row + 1 - 2 * lax.rem(row, 2)), (dp, col, lax.rem(row + n_row // 2, n_row)), (dp, lax.rem(col + 1, n_col), row))

    def plane_peer(step):
        other = lax.rem(me + step, plane)
        return other, (dp, lax.div(other, n_row), lax.rem(other, n_row))

    def remote(src, dst, send, recv, device):
        return pltpu.make_async_remote_copy(
            src_ref=src, dst_ref=dst, send_sem=send, recv_sem=recv, device_id=device, device_id_type=MESH)

    def first_part(tile, j):
        r0, r_n, c0, c_n = PARTS[j]
        at = (tile, pl.ds(r0, r_n), pl.ds(c0, c_n))
        return remote(part.at[at], peer.at[at], sub_send.at[j], sub_recv.at[j], across)

    def bulk(tile):
        return remote(part.at[tile], peer.at[tile], bulk_send.at[tile], bulk_recv.at[tile], across)

    def gather(tile):
        at = (slice(None), pl.ds(pl.multiple_of(tile * TN, TN), TN))
        return remote(w_outs[0].at[at], w_outs[0].at[at], gather_sem.at[0], gather_sem.at[1], across)

    def z_copy(n, buf, slot):
        return remote(buf.at[slot], buf.at[slot], z_send.at[n], z_recv.at[n], across)

    half = geo.tokens // HALVES

    def first_x(n, pieces, c, c0, c_n):
        rows = pl.ds(c * (geo.tokens // pieces), geo.tokens // pieces)
        at = (rows, pl.ds(c0, c_n))
        return pltpu.make_async_copy(x_refs[0].at[at], xbuf.at[0].at[at], first_sem.at[n, c])

    def first_y(n, pieces, c, c0, c_n):
        rows = pl.ds(c * (geo.tokens // pieces), geo.tokens // pieces)
        columns = pl.ds(pl.multiple_of(other * TN + c0, LANES), c_n)
        return pltpu.make_async_copy(dy_refs[0].at[rows, columns], ybuf.at[0, rows, pl.ds(c0, c_n)], first_sem.at[n, c])

    n_steps = geo.n_tiles - 1

    def tile_of(s):
        past_zero = lax.div(s + (n_steps - 1), n_steps)
        past_one = lax.div(s + (n_steps - 2), n_steps)
        return s + 1 + (1 - past_zero) - (past_zero - past_one) * (2 - own)

    def slot_of(s):
        return lax.rem(s + 1, 2)

    def load(s):
        tile, slot = tile_of(s), slot_of(s)
        for first, count, m_tiles, x_ref, y_ref in geo.groups(x_refs, dy_refs):
            @pl.when(jnp.logical_and(tile >= first, tile < first + count))
            def _():
                local = tile - first
                m_at = local if m_tiles > 1 else 0
                n_at = 0 if m_tiles > 1 else local
                for h in range(HALVES):
                    rows = pl.ds(h * half, half)
                    pltpu.make_async_copy(
                        x_ref.at[rows, pl.ds(pl.multiple_of(m_at * TM, TM), TM)],
                        xbuf.at[slot, rows], x_sem.at[slot, h]).start()
                    pltpu.make_async_copy(
                        y_ref.at[rows, pl.ds(pl.multiple_of(n_at * TN, TN), TN)],
                        ybuf.at[slot, rows], y_sem.at[slot, h]).start()

    def load_done(slot, h):
        rows = pl.ds(h * half, half)
        pltpu.make_async_copy(x_refs[0].at[rows, pl.ds(0, TM)], xbuf.at[slot, rows], x_sem.at[slot, h]).wait()
        pltpu.make_async_copy(dy_refs[0].at[rows, pl.ds(0, TN)], ybuf.at[slot, rows], y_sem.at[slot, h]).wait()

    def contract(x, y):
        return lax.dot_general(x, y, (((0,), (0,)), ((), ())), preferred_element_type=F32)

    first_loads = (
        (4, lambda c: (first_x(0, 4, c, 0, 128), first_y(1, 4, c, 0, 128))),
        (2, lambda c: (first_y(2, 2, c, 128, 128),)),
        (2, lambda c: (first_x(3, 2, c, 128, 128),)),
        (2, lambda c: (first_y(4, 2, c, 256, 256),)),
    )
    def start_first(j):
        pieces, copies_of = first_loads[j]
        for c in range(pieces):
            for copy in copies_of(c):
                copy.start()

    for j in range(4):
        start_first(j)
    starts = {(2, 0): lambda: load(0)}

    barrier = pltpu.get_barrier_semaphore()
    for device in (across, *near):
        pl.semaphore_signal(barrier, inc=1, device_id=device, device_id_type=MESH)


    for j, (pieces, copies_of) in enumerate(first_loads):
        r0, r_n, c0, c_n = PARTS[j]
        at = (other, pl.ds(r0, r_n), pl.ds(c0, c_n))
        for c in range(pieces):
            for copy in copies_of(c):
                copy.wait()
            if (j, c) in starts:
                starts[j, c]()
            rows = pl.ds(c * (geo.tokens // pieces), geo.tokens // pieces)
            term = contract(xbuf[0, rows, pl.ds(r0, r_n)], ybuf[0, rows, pl.ds(c0, c_n)])
            part[at] = term if c == 0 else part[at] + term
        if j == 0:
            pl.semaphore_wait(barrier, 1 + len(near))
        if j in (2,):
            @pl.when(lax.rem(row, 2) == 0)
            def _():
                first_part(other, j).start()
        else:
            if j == 3:
                @pl.when(lax.rem(row, 2) == 1)
                def _():
                    for held in (2,):
                        first_part(other, held).start()
            first_part(other, j).start()
    w_copies = [pltpu.make_async_copy(w_refs[i], w_outs[i], w_sem.at[i]) for i in range(4)]
    w_copies += [pltpu.make_async_copy(a, b, small_sem.at[i]) for i, (a, b) in enumerate(zip(small_refs, small))]

    def tiles(lo, hi):
        @pl.loop(lo, hi)
        def _(s):
            tile, slot = tile_of(s), slot_of(s)

            @pl.when(s + 1 < n_steps)
            def _():
                load(s + 1)

            for h in range(HALVES):
                load_done(slot, h)
                rows = pl.ds(h * half, half)
                term = contract(xbuf[slot, rows, :], ybuf[slot, rows, :])
                if h == 0:
                    part[tile] = term
                else:
                    part[tile] += term

            @pl.when(s != 1)
            def _():
                bulk(tile).start()

    def w_at(i, t, r):
        if geo.wide(i):
            return pl.ds(r, RB), pl.ds(pl.multiple_of(t * TN, TN), TN)
        return pl.ds(t * TM + r, RB), pl.ds(0, TN)

    def stat_at(i, t, r):
        return pl.ds(r, RB) if geo.wide(i) else pl.ds(t * TM + r, RB)

    def stat_tile(i, t, rows_ref, accumulate, col_sum):
        tile = geo.mats[i][0] + t

        def step(b, acc):
            r = pl.multiple_of(b * RB, RB)
            grad = part[tile, pl.ds(r, RB), :] + peer[tile, pl.ds(r, RB), :]
            peer[tile, pl.ds(r, RB), :] = grad
            sq = grad * grad + EPS_ONE
            at = stat_at(i, t, r)
            if accumulate:
                rows_ref[at, :] += fold_lanes(sq)
            else:
                rows_ref[at, :] = fold_lanes(sq)
            return acc + fold_rows(sq)

        return lax.fori_loop(0, TM // RB, step, col_sum)

    def norm_tile(i, t, acc):
        tile = geo.mats[i][0] + t
        scale = brow[:, pl.ds(pl.multiple_of(t * TN, TN), TN)] if geo.wide(i) else brow[:, pl.ds(0, TN)]

        def step(b, acc):
            r = pl.multiple_of(b * RB, RB)
            upd = peer[tile, pl.ds(r, RB), :] * scale
            lane_scale = acol[stat_at(i, t, r), :]
            return acc + fold_rows(fold_lanes(upd * upd) * lane_scale * lane_scale)

        return lax.fori_loop(0, TM // RB, step, acc)

    def write_tile(i, t, step_size):
        tile = geo.mats[i][0] + t
        scale = brow[:, pl.ds(pl.multiple_of(t * TN, TN), TN)] if geo.wide(i) else brow[:, pl.ds(0, TN)]
        scale = scale * step_size

        def step(b, _):
            r = pl.multiple_of(b * RB, RB)
            upd = peer[tile, pl.ds(r, RB), :] * scale
            lane_scale = jnp.concatenate([acol[stat_at(i, t, r), :]] * (TN // LANES), axis=1)
            w_outs[i][w_at(i, t, r)] = w_outs[i][w_at(i, t, r)] - upd * lane_scale
            return 0

        lax.fori_loop(0, TM // RB, step, 0)

    def weight_squares(i):
        acc = jnp.zeros((8, LANES), F32)
        for t in range(geo.mats[i][1]):
            def step(b, acc):
                w = w_outs[i][w_at(i, t, pl.multiple_of(b * RB, RB))]
                return acc + fold_rows(fold_lanes(w * w))

            acc = lax.fori_loop(0, TM // RB, step, acc)
        w_sq[pl.ds(i, 1), :] = row_sum_of(acc)

    def row_totals(rows_ref, j):
        return row_sum_of(jnp.transpose(rows_ref[pl.ds(j, LANES), :]))

    def exchange(i, buf, send, recv):
        copies = []
        for step in range(1, plane):
            device = plane_peer(step)[1]
            copies.append(remote(buf.at[me], buf.at[me], send.at[i, step], recv.at[i, me], device))
        for copy in copies:
            copy.start()
        for step in range(1, plane):
            there, device = plane_peer(step)
            remote(buf.at[there], buf.at[there], send.at[i, step], recv.at[i, there], device).wait_recv()
        return copies

    def sizes(i):
        _, _, m_loc, n_loc = geo.mats[i]
        return m_loc, n_loc, m_loc + n_loc, m_loc * n_row, n_loc * n_col

    def round_one(i, z_part):
        m_loc, n_loc, tail, m_total, n_total = sizes(i)
        one = msg_one[i]
        r_fold = jnp.zeros((1, LANES), F32)
        for j in range(0, m_loc, LANES):
            total = row_totals(rowpart, j)
            if z_part:
                total = total + (zmsg_one[0, :, pl.ds(j, LANES)] + zmsg_one[1, :, pl.ds(j, LANES)])
            one[pl.ds(me, 1), :, pl.ds(j, LANES)] = total[None]
            r_fold = r_fold + r_refs[i][:, pl.ds(j, LANES)]
        one[pl.ds(me, 1), :, pl.ds(m_loc, n_loc)] = colpart[:, pl.ds(0, n_loc)][None]
        if z_part:
            for t in range(2):
                one[pl.ds(me, 1), :, pl.ds(m_loc + t * TN, TN)] = zmsg_one[t, :, pl.ds(m_loc, TN)][None]
        one[pl.ds(me, 1), :, pl.ds(tail, LANES)] = r_fold[None]
        one[pl.ds(me, 1), :, pl.ds(tail + LANES, LANES)] = w_sq[pl.ds(i, 1), :][None]
        sent = exchange(i, one, one_send, one_recv)

        row_sum = one[row, :, pl.ds(0, m_loc)]
        for j in range(1, n_col):
            row_sum = row_sum + one[j * n_row + row, :, pl.ds(0, m_loc)]
        col_sum = one[col * n_row, :, pl.ds(m_loc, n_loc)]
        for j in range(1, n_row):
            col_sum = col_sum + one[col * n_row + j, :, pl.ds(m_loc, n_loc)]
        new_row = beta_two * r_refs[i][...] + (1.0 - beta_two) * (row_sum / n_total)
        new_col = beta_two * c_refs[i][...] + (1.0 - beta_two) * (col_sum / m_total)
        r_outs[i][...] = new_row
        c_outs[i][...] = new_col

        old_fold = jnp.zeros((1, LANES), F32)
        sq_fold = jnp.zeros((1, LANES), F32)
        for j in range(plane):
            sq_fold = sq_fold + fold_lanes(one[j, :, pl.ds(0, m_loc)])
            if j < n_row:
                old_fold = old_fold + one[j, :, pl.ds(tail, LANES)]
        total = lane_sum(beta_two * old_fold + (1.0 - beta_two) * (sq_fold / n_total))

        row_scale = jnp.sqrt(total) / jnp.sqrt(new_row)
        for j in range(0, m_loc, LANES):
            acol[pl.ds(j, LANES), :] = jnp.transpose(jnp.broadcast_to(row_scale[:, j:j + LANES], (LANES, LANES)))
        brow[:, pl.ds(0, n_loc)] = 1.0 / jnp.sqrt(new_col)
        return sent

    def round_two(i, upd_sq):
        _, _, tail, m_total, n_total = sizes(i)
        one, two = msg_one[i], msg_two.at[i]
        two[pl.ds(me, 1)] = upd_sq[None]
        sent = exchange(i, two, two_send, two_recv)
        upd_fold, w_fold = two[0], one[0, :, pl.ds(tail + LANES, LANES)]
        for j in range(1, plane):
            upd_fold = upd_fold + two[j]
            w_fold = w_fold + one[j, :, pl.ds(tail + LANES, LANES)]
        upd_rms = jnp.sqrt(lane_sum(upd_fold) / (m_total * n_total))
        w_rms = jnp.sqrt(lane_sum(w_fold) / (m_total * n_total))
        return rho_step * jnp.maximum(EPS_TWO, w_rms) / jnp.maximum(1.0, upd_rms / clip_thr), sent

    none = jnp.zeros((8, TN), F32)
    no_lanes = jnp.zeros((8, LANES), F32)
    m_gate = geo.mats[0][2]

    tiles(0, 4)

    for copy in w_copies:
        copy.start()

    for n in range(2):
        for device in near:
            pl.semaphore_signal(near_sem.at[n], inc=1, device_id=device, device_id_type=MESH)
        pl.semaphore_wait(near_sem.at[n], len(near))

    for copy in w_copies:
        copy.wait()
    beta_two, rho_step, clip_thr = hyper[0], hyper[1], hyper[2]
    for i in range(4):
        weight_squares(i)
    for j in range(len(PARTS)):
        first_part(own, j).wait_recv()
    own_col = stat_tile(0, own, rowpart_own, False, none)
    for j in range(0, TM, LANES):
        zmsg_one[pl.ds(own, 1), :, pl.ds(j, LANES)] = row_totals(rowpart_own, j)[None]
    zmsg_one[pl.ds(own, 1), :, pl.ds(m_gate, TN)] = row_sum_of(own_col)[None]
    z_copy(0, zmsg_one, own).start()

    tiles(4, 6)

    shared = range(2, geo.mats[0][1])
    for t in shared:
        bulk(t).wait_recv()
        colpart[:, pl.ds(t * TN, TN)] = row_sum_of(stat_tile(0, t, rowpart, t > 2, none))
    z_copy(0, zmsg_one, other).wait_recv()
    gate_sent = round_one(0, True)
    zmsg_two[pl.ds(own, 1)] = row_sum_of(norm_tile(0, own, no_lanes))[None]
    z_copy(1, zmsg_two, own).start()

    tiles(6, 8)

    upd_sq = no_lanes
    for t in shared:
        upd_sq = norm_tile(0, t, upd_sq)
    z_copy(1, zmsg_two, other).wait_recv()
    step_size, sent = round_two(0, row_sum_of(upd_sq) + (zmsg_two[0] + zmsg_two[1]))
    gate_sent += sent
    write_tile(0, own, step_size)
    for t in shared:
        write_tile(0, t, step_size)

    tiles(8, geo.n_tiles - 1)
    gather(own).start()

    for i in range(1, 4):
        first, count, m_loc, n_loc = geo.mats[i]
        col_sum = none
        for t in range(count):
            bulk(first + t).wait_recv()
            if geo.wide(i):
                colpart[:, pl.ds(t * TN, TN)] = row_sum_of(stat_tile(i, t, rowpart, t > 0, none))
            else:
                col_sum = stat_tile(i, t, rowpart, False, col_sum)
        if not geo.wide(i):
            colpart[:, pl.ds(0, TN)] = row_sum_of(col_sum)
        sent_one = round_one(i, False)
        upd_sq = no_lanes
        for t in range(count):
            upd_sq = norm_tile(i, t, upd_sq)
        step_size, sent_two = round_two(i, row_sum_of(upd_sq))
        for t in range(count):
            write_tile(i, t, step_size)
        for copy in sent_one + sent_two:
            copy.wait_send()

    for copy in gate_sent:
        copy.wait_send()
    z_copy(0, zmsg_one, own).wait_send()
    z_copy(1, zmsg_two, own).wait_send()
    for j in range(len(PARTS)):
        first_part(other, j).wait_send()

    @pl.loop(2, geo.n_tiles)
    def _(tile):
        bulk(tile).wait_send()

    gather(own).wait_send()
    gather(other).wait_recv()


def write_out(*refs):
    copies = [pltpu.make_async_copy(refs[i], refs[12 + i], refs[24].at[i]) for i in range(12)]
    for copy in copies:
        copy.start()
    for copy in copies:
        copy.wait()


class Geometry:
    def __init__(self, n_row, n_col, tokens, blocks):
        self.n_row, self.n_col = n_row, n_col
        self.tokens = tokens
        self.mats, first = [], 0
        for m_loc, n_loc in blocks:
            count = (m_loc // TM) * (n_loc // TN)
            self.mats.append((first, count, m_loc, n_loc))
            first += count
        self.n_tiles = first

    def wide(self, i):
        return self.mats[i][2] == TM

    def groups(self, x_refs, dy_refs):
        for (first, count, m_loc, _), x_ref, y_ref in zip(self.mats, x_refs, dy_refs):
            yield first, count, m_loc // TM, x_ref, y_ref


def solution(mesh):
    n_row, n_col = mesh.shape["row"], mesh.shape["col"]
    plane = n_row * n_col
    act_spec = P('dp', 'row')
    grad_spec = P('dp', 'col')
    w_spec = P('row', 'col')
    row_spec = P('row')
    col_spec = P('col')
    in_specs = (act_spec, grad_spec, act_spec, grad_spec, grad_spec, act_spec, grad_spec,
                w_spec, w_spec, w_spec, w_spec,
                row_spec, col_spec, row_spec, col_spec, row_spec, col_spec, row_spec, col_spec, P())
    out_specs = (w_spec, row_spec, col_spec) * 4

    def per_device(x_attn, dy_attn, x_mlp, dy_gate, dy_up, h_mlp, dy_out, w_attn, w_gate, w_up, w_down,
                   r_attn, c_attn, r_gate, c_gate, r_up, c_up, r_down, c_down, hyper_params):
        weights = (w_gate, w_up, w_down, w_attn)
        rows = [v.reshape(1, -1) for v in (r_gate, r_up, r_down, r_attn)]
        cols = [v.reshape(1, -1) for v in (c_gate, c_up, c_down, c_attn)]
        blocks = [w.shape for w in weights]
        geo = Geometry(n_row, n_col, x_attn.shape[0], blocks)
        results = (*weights, *rows, *cols)
        hbm = pl.BlockSpec(memory_space=pl.ANY)
        vmem = pl.BlockSpec(memory_space=pltpu.VMEM)
        dma = pltpu.SemaphoreType.DMA
        max_m, max_n = max(b[0] for b in blocks), max(b[1] for b in blocks)

        def body(*refs):
            xs = (refs[0], refs[0], refs[1], refs[2])
            kernel(geo, xs, refs[3:7], refs[7:11], refs[11:20], refs[20:24], refs[24:28], refs[28:32], refs[32:41],
                   *refs[41:51], refs[51:55], *refs[55:])

        outs = pl.pallas_call(
            body,
            out_shape=tuple(pltpu.VMEM(v.shape, F32) for v in results),
            in_specs=[hbm] * 20,
            out_specs=(vmem,) * 12,
            scratch_shapes=[pltpu.VMEM(v.shape, F32) for v in (*rows, *cols)] + [
                pltpu.SMEM((3,), F32),
                pltpu.VMEM((2, geo.tokens, TM), jnp.bfloat16),
                pltpu.VMEM((2, geo.tokens, TN), jnp.bfloat16),
                pltpu.VMEM((geo.n_tiles, TM, TN), F32),
                pltpu.VMEM((geo.n_tiles, TM, TN), F32),
                pltpu.VMEM((max_m, LANES), F32),
                pltpu.VMEM((TM, LANES), F32),
                pltpu.VMEM((max_m, LANES), F32),
                pltpu.VMEM((1, max_n), F32),
                pltpu.VMEM((1, max_n), F32),
                pltpu.VMEM((8, LANES), F32),
            ] + [pltpu.VMEM((plane, 1, m + n + 2 * LANES), F32) for m, n in blocks] + [
                pltpu.VMEM((4, plane, 1, LANES), F32),
                pltpu.VMEM((2, 1, TM + TN), F32),
                pltpu.VMEM((2, 1, LANES), F32),
                dma((2, HALVES)), dma((2, HALVES)), dma((5, 4)), dma((4,)),
                dma((len(PARTS),)), dma((len(PARTS),)), dma((geo.n_tiles,)), dma((geo.n_tiles,)), dma((2,)),
                dma((4, plane)), dma((4, plane)), dma((4, plane)), dma((4, plane)), dma((2,)), dma((2,)), dma((9,)),
                pltpu.SemaphoreType.REGULAR((2,)),
            ],
            compiler_params=pltpu.CompilerParams(
                collective_id=0, has_side_effects=True, vmem_limit_bytes=48 << 20),
            name="adafactor_step",
        )(x_mlp, h_mlp, x_attn, dy_gate, dy_up, dy_out, dy_attn, *weights, *rows, *cols, hyper_params)
        outs = pl.pallas_call(
            write_out,
            out_shape=tuple(jax.ShapeDtypeStruct(v.shape, F32) for v in results),
            in_specs=[vmem] * 12,
            out_specs=(hbm,) * 12,
            scratch_shapes=[dma((12,))],
            compiler_params=pltpu.CompilerParams(vmem_limit_bytes=1 << 20),
            name="write_out",
        )(*[pltpu.with_memory_space_constraint(v, pltpu.VMEM) for v in outs])
        w_new, r_new, c_new = outs[:4], outs[4:8], outs[8:]
        result = []
        for i in (3, 0, 1, 2):
            result += [w_new[i], r_new[i].reshape(-1), c_new[i].reshape(-1)]
        return tuple(result)

    return jax.shard_map(per_device, mesh=mesh, in_specs=in_specs, out_specs=out_specs, check_vma=False)
```
